32 devices in a mesh: groups: 2 (over x), seq: 16 (over z, y, core).
Axes of the slice: x: 2, y: 2, z: 4, core: 2. Of those that a mesh axis runs over, the one named last changes fastest.
Arguments:
- query_block: bfloat16 [512, 4096], P(('groups', 'seq')), parts along dimension 0, may hold values from -112 to 112
- cache_keys: bfloat16 [8192, 2048], P(('groups', 'seq')), parts along dimension 0, may hold values from -4 to 4
- stored_values: bfloat16 [8192, 2048], P(('groups', 'seq')), parts along dimension 0, may hold values from -6 to 6
- live_counts: int32 [32], P(('groups', 'seq')), parts along dimension 0, may hold values from 128 to 256
- first_position: int32 [2], P('groups'), parts along dimension 0, may hold values from 0 to 3840
- out_weight: bfloat16 [4096, 5376], P('seq'), may hold values from -0.09375 to 0.09375
Outputs:
- attended: bfloat16 [512, 5376], P(('groups', 'seq')), parts along dimension 0
The draws below stay inside these ranges and needn't reach their ends.
There are 2 independent parts, one for each index of `groups`. The reference program is written for one: setup_inputs(seed, part) draws one part's arguments, and reference() takes and returns one part's arrays. A program takes and returns all parts, laid end to end along the dimension named above; an argument that names none is the same for every part. Nothing has to cross between parts.
Inputs may be any that keep to these rules, and one draw needn't show every extreme that they name: `live_counts`: the live slots of a block are its first ones.
All inputs are finite; a program needn't handle non-finite values.
Results may differ from the reference program's by a relative error of at most 0.0058.
Values may be sent and summed in bfloat16 or wider, within the bound.
No kernel may reach another device: no remote copies, remote signals or barrier semaphores. Data moves between devices by JAX's collectives and lax.ppermute only.
A program may use at most 64 MiB of HBM per device.

```python
import jax
import jax.numpy as jnp
from jax import lax

D = 5376
QUERY_HEADS = 32
KEY_VALUE_HEADS = 16
HEAD_SIZE = 128
K_DEV = 256
QUERIES = 256
SLOT_COUNT = 4096
N_SEQ = 16


def draw_pair(key):
    folded = jax.random.fold_in(key, 4242)
    key_sample = jax.random.fold_in(folded, 0)
    query_draw = jax.random.fold_in(folded, 1)
    pick_draw = jax.random.fold_in(folded, 2)
    sign_draw = jax.random.fold_in(folded, 4)
    cache_entries = jnp.clip(jax.random.normal(key_sample, (SLOT_COUNT, KEY_VALUE_HEADS * HEAD_SIZE), jnp.float32), -4.0, 4.0)
    queries = jnp.clip(3.0 * jax.random.normal(query_draw, (QUERIES, QUERY_HEADS * HEAD_SIZE), jnp.float32), -12.0, 12.0)
    signs = jnp.where(jax.random.bernoulli(sign_draw, 0.5, (KEY_VALUE_HEADS * HEAD_SIZE,)), 4.0, -4.0).astype(jnp.float32)
    cache_entries = cache_entries.at[0].set(signs)
    cache_entries = cache_entries.at[1].set(0.99 * signs)
    chosen = jax.random.permutation(pick_draw, QUERIES)[:3]
    targets = jnp.array([120.0, 200.0, 300.0], jnp.float32)
    strengths = targets * 168.0 ** 0.5 / (16.0 * HEAD_SIZE)
    keys_per_head = jnp.repeat(signs.reshape(KEY_VALUE_HEADS, HEAD_SIZE), QUERY_HEADS // KEY_VALUE_HEADS, axis=0).reshape(QUERY_HEADS * HEAD_SIZE)
    queries = queries.at[chosen].set(strengths[:, None] * keys_per_head[None, :])
    return (queries, cache_entries)


def draw_query_block(key, part):
    queries, cache_entries = draw_pair(key)
    return queries.astype(jnp.bfloat16)


def draw_cache_keys(key, part):
    queries, cache_entries = draw_pair(key)
    return cache_entries.astype(jnp.bfloat16)


def with_ends(entries, stream_key, low, high):
    longest = entries.shape.index(max(entries.shape))
    spots = []
    for shift in (0, 1):
        where = [jax.random.randint(jax.random.fold_in(stream_key, axis), (), 0, length) for axis, length in enumerate(entries.shape)]
        where[longest] = (where[longest] + shift) % entries.shape[longest]
        spots.append(tuple(where))
    return entries.at[spots[0]].set(low).at[spots[1]].set(high)


def steps_of(rng, dims, cuts, least, high):
    level = 1.0
    for position, parts in cuts:
        steps = jax.random.uniform(jax.random.fold_in(jax.random.fold_in(rng, 6), position), (parts,), jnp.float32, least / len(cuts), high / len(cuts))
        level = level * jnp.repeat(jnp.exp(steps), dims[position] // parts).reshape((-1,) + (1,) * (len(dims) - 1 - position))
    return level


def bell_draw(rng, dims, width, most, pieces=(), kind=jnp.bfloat16):
    factor_of = steps_of(rng, dims, pieces, -0.22, 0.18) if pieces else 1.0
    result = jax.random.normal(rng, dims, jnp.float32) * width * factor_of
    return jnp.minimum(jnp.maximum(result, -most), most).astype(kind)


def setup_inputs(seed: int = 0, part: int = 0) -> dict:
    streams_of = jax.random.split(jax.random.key(seed), 7)
    part_splits = jax.random.split(jax.random.fold_in(streams_of[6], part), 7)
    return {
        "query_block": draw_query_block(jax.random.fold_in(jax.random.fold_in(streams_of[6], part), 71), part),
        "cache_keys": draw_cache_keys(jax.random.fold_in(jax.random.fold_in(streams_of[6], part), 71), part),
        "stored_values": bell_draw(part_splits[2], (SLOT_COUNT, KEY_VALUE_HEADS * HEAD_SIZE), 1.0, 6.0, ((0, 16),)),
        "live_counts": with_ends(jax.random.randint(part_splits[3], (N_SEQ,), K_DEV // 2, K_DEV + 1), jax.random.fold_in(part_splits[3], 1), K_DEV // 2, K_DEV).astype(jnp.int32),
        "first_position": jax.random.randint(part_splits[4], (1,), 0, SLOT_COUNT - QUERIES + 1).astype(jnp.int32),
        "out_weight": bell_draw(streams_of[5], (QUERY_HEADS * HEAD_SIZE, D), (QUERY_HEADS * HEAD_SIZE) ** -0.5, 0.09375, ((0, 16),)),
    }


score_scale = 168.0 ** -0.5
masked_value = -1e30


def head_partial(query_cols, key_cols, value_cols, allowed, group_width):
    row_count = query_cols.shape[0]
    grouped = query_cols.reshape(row_count, group_width, HEAD_SIZE).astype(jnp.float32)
    scores = jnp.einsum("rgd,kd->grk", grouped, key_cols.astype(jnp.float32), precision=lax.Precision.HIGHEST) * score_scale
    row_best = jnp.max(jnp.where(allowed[None], scores, masked_value), axis=2)
    shifted = jnp.where(allowed[None], scores - row_best[:, :, None], -jnp.inf)
    weights = jnp.exp(shifted)
    weight_sum = jnp.sum(weights, axis=2)
    safe_total = jnp.where(weight_sum > 0, weight_sum, 1.0)
    rounded = lax.optimization_barrier(weights.astype(jnp.bfloat16)).astype(jnp.float32)
    weighted = jnp.einsum("grk,kd->grd", rounded, value_cols.astype(jnp.float32), precision=lax.Precision.HIGHEST)
    value_partial_sum = (weighted / safe_total[:, :, None]).astype(jnp.bfloat16)
    log_sum_exp = jnp.where(weight_sum > 0, row_best + jnp.log(safe_total), masked_value)
    return value_partial_sum, log_sum_exp


def source_partial(query_block, cache_keys, stored_values, live_counts, first_position, source):
    key_start = (source * K_DEV).astype(jnp.int32)
    key_rows = lax.dynamic_slice_in_dim(cache_keys, key_start, K_DEV, 0)
    value_rows = lax.dynamic_slice_in_dim(stored_values, key_start, K_DEV, 0)
    key_index = lax.iota(jnp.int32, K_DEV)
    query_pos = first_position[0] + lax.iota(jnp.int32, QUERIES)
    allowed = (key_index[None, :] < live_counts[source]) & (key_start + key_index[None, :] <= query_pos[:, None])
    group_width = QUERY_HEADS // KEY_VALUE_HEADS
    partial_list = []
    logsum_list = []
    for key_value_head in range(KEY_VALUE_HEADS):
        query_cols = query_block[:, key_value_head * group_width * HEAD_SIZE:(key_value_head + 1) * group_width * HEAD_SIZE]
        key_cols = key_rows[:, key_value_head * HEAD_SIZE:(key_value_head + 1) * HEAD_SIZE]
        value_cols = value_rows[:, key_value_head * HEAD_SIZE:(key_value_head + 1) * HEAD_SIZE]
        value_partial_sum, log_sum_exp = head_partial(query_cols, key_cols, value_cols, allowed, group_width)
        partial_list.append(value_partial_sum)
        logsum_list.append(log_sum_exp)
    value_partial_sum = jnp.transpose(jnp.stack(partial_list), (2, 0, 1, 3)).reshape(QUERIES, QUERY_HEADS, HEAD_SIZE)
    log_sum_exp = jnp.transpose(jnp.stack(logsum_list), (2, 0, 1)).reshape(QUERIES, QUERY_HEADS)
    return value_partial_sum, log_sum_exp


def reference(query_block, cache_keys, stored_values, live_counts, first_position, out_weight):
    def one_source(source):
        return source_partial(query_block, cache_keys, stored_values, live_counts, first_position, source)

    partials, logsums = lax.map(one_source, jnp.arange(N_SEQ, dtype=jnp.int32))
    largest = jnp.max(logsums, axis=0)
    scales = jnp.exp(logsums - largest[None])
    merged = (jnp.sum(scales[..., None] * partials.astype(jnp.float32), axis=0) / jnp.sum(scales, axis=0)[..., None]).astype(jnp.bfloat16)
    per_group = QUERY_HEADS // N_SEQ
    flattened = merged.reshape(QUERIES, QUERY_HEADS * HEAD_SIZE)

    def add_group(group, running):
        offset = (group * (per_group * HEAD_SIZE)).astype(jnp.int32)
        head_columns = lax.dynamic_slice_in_dim(flattened, offset, per_group * HEAD_SIZE, 1)
        weight_rows = lax.dynamic_slice_in_dim(out_weight, offset, per_group * HEAD_SIZE, 0)
        projected = jnp.dot(head_columns, weight_rows, preferred_element_type=jnp.float32)
        return running + projected

    summed = lax.fori_loop(jnp.int32(0), jnp.int32(N_SEQ), add_group, jnp.zeros((QUERIES, D), jnp.float32))
    return summed.astype(jnp.bfloat16)
```

```python
import functools

import jax
import jax.numpy as jnp
from jax import lax
from jax.experimental import pallas as pl
from jax.experimental.pallas import tpu as pltpu
from jax.sharding import PartitionSpec as P

QUERY_HEADS = 32
KEY_VALUE_HEADS = 16
HEAD_SIZE = 128
INNER = 4
CHUNKS = 3

score_scale = 168.0 ** (-0.5)
masked_value = -1e30
log2e = 1.4426950408889634
ln2 = 0.6931471805599453


bf16 = jnp.bfloat16
f32 = jnp.float32
VM = pltpu.MemorySpace.VMEM
SM = pltpu.MemorySpace.SMEM


def vspec():
    return pl.BlockSpec(memory_space=VM)


def sspec():
    return pl.BlockSpec(memory_space=SM)


def place():
    me = lax.axis_index("seq")
    return me, lax.shift_right_logical(me, 2), lax.bitwise_and(me, 3)


def call(kernel, name, ins, outs, scratch=(), scalars=0, flops=0):
    in_specs = [sspec()] * scalars + [vspec()] * (len(ins) - scalars)
    moved = sum(a.size * a.dtype.itemsize for a in list(ins) + list(outs))
    return pl.pallas_call(
        kernel,
        out_shape=tuple(outs),
        in_specs=in_specs,
        out_specs=tuple(vspec() for _ in outs),
        scratch_shapes=list(scratch),
        name=name,
        cost_estimate=pl.CostEstimate(flops=flops, transcendentals=0, bytes_accessed=moved),
    )(*ins)


def split_queries_kernel(q_ref, *out_refs, outer, width):
    me, z, r = place()
    for k, out in enumerate(out_refs):
        for zz in range(outer):
            col = (zz * INNER + lax.bitwise_xor(r, k)) * width
            out[zz] = q_ref[:, pl.ds(pl.multiple_of(col, width), width)]


def split_cache_kernel(live_ref, k_ref, v_ref, *out_refs, offsets, copies):
    me, z, r = place()
    keys = k_ref.shape[0]
    live = jnp.full((16, HEAD_SIZE), live_ref[0], jnp.int32).astype(f32).astype(bf16)
    for k, out in enumerate(out_refs):
        for i, kk in enumerate(offsets):
            head = lax.bitwise_xor(z, kk) * INNER + lax.bitwise_xor(r, k)
            col = pl.multiple_of((head // copies) * HEAD_SIZE, HEAD_SIZE)
            out[i, 0:keys, :] = k_ref[:, pl.ds(col, HEAD_SIZE)]
            out[i, keys:2 * keys, :] = v_ref[:, pl.ds(col, HEAD_SIZE)]
            out[i, 2 * keys:2 * keys + 16, :] = live


def attention_kernel(first_ref, *refs, outer, offsets, rows_all, keys, heads, width):
    ys = refs[:outer]
    kvs = refs[outer:outer + INNER]
    outs = refs[outer + INNER:outer + INNER + len(offsets)]
    bias_ref, q_ref = refs[outer + INNER + len(offsets):]
    me, z, r = place()
    rows = rows_all // (outer * INNER)
    q_pos = first_ref[0] + lax.broadcasted_iota(jnp.int32, (rows_all, keys), 0)
    lane = lax.broadcasted_iota(jnp.int32, (rows_all, keys), 1)
    lane_f = lane.astype(f32)
    for k in range(INNER):
        start = (z * INNER + lax.bitwise_xor(r, k)) * keys
        live = kvs[k][0, 2 * keys:2 * keys + 1, :].astype(f32)
        live = jnp.concatenate([live] * (keys // HEAD_SIZE), axis=1)
        allowed = (lane_f < live) & (start + lane <= q_pos)
        bias_ref[:, k * keys:(k + 1) * keys] = jnp.where(allowed, 0.0, masked_value)
    column = lax.broadcasted_iota(jnp.int32, (rows_all, 128), 1)
    for i, kk in enumerate(offsets):
        zz = lax.bitwise_xor(z, kk)
        for k2 in range(outer):
            for k in range(INNER):
                src = lax.bitwise_xor(z, k2) * INNER + lax.bitwise_xor(r, k)
                at = pl.multiple_of(src * rows, rows)
                q_ref[pl.ds(at, rows), :] = ys[k2][k, zz].astype(f32)
        stats = jnp.zeros((rows_all, 128), f32)
        for h in range(heads):
            cols = slice(h * HEAD_SIZE, (h + 1) * HEAD_SIZE)
            query = q_ref[:, cols].astype(bf16)
            scores = []
            for k in range(INNER):
                part = lax.dot_general(
                    query, kvs[k][i, 0:keys, :], (((1,), (1,)), ((), ())),
                    preferred_element_type=f32,
                )
                scores.append(part * (score_scale * log2e) + bias_ref[:, k * keys:(k + 1) * keys])
            top = functools.reduce(jnp.maximum, scores)
            best = jnp.maximum(jnp.max(top, axis=1, keepdims=True), -1e29)
            acc = jnp.zeros((rows_all, HEAD_SIZE), f32)
            sums = jnp.zeros((rows_all, keys), f32)
            for k in range(INNER):
                weights = jnp.exp2(scores[k] - best)
                sums = sums + weights
                acc = acc + jnp.dot(
                    weights.astype(bf16), kvs[k][i, keys:2 * keys, :], preferred_element_type=f32
                )
            total = jnp.sum(sums, axis=1, keepdims=True)
            safe = jnp.where(total > 0, total, 1.0)
            outs[i][0:rows_all, cols] = (acc / safe).astype(bf16)
            logsum = jnp.where(total > 0, best * ln2 + jnp.log(safe), masked_value)
            high = logsum.astype(bf16).astype(f32)
            rest = logsum - high
            mid = rest.astype(bf16).astype(f32)
            low = rest - mid
            for p, piece in enumerate((high, mid, low)):
                stats = jnp.where(column == p * heads + h, piece, stats)
        turned = stats.T
        pieces = rows_all // width
        per = 16 // pieces
        block = [turned[0:per, j * width:(j + 1) * width] for j in range(pieces)]
        block = block[0] if pieces == 1 else jnp.concatenate(block, axis=0)
        outs[i][rows_all:rows_all + 16, :] = block.astype(bf16)


def merge_kernel(*refs, sources, rows_all, heads, width):
    parts = refs[:sources]
    out, turn_ref = refs[sources:]
    pieces = rows_all // width
    per = 16 // pieces
    logs = []
    for part in parts:
        block = part[rows_all:rows_all + 16, :].astype(f32)
        block = [block[j * per:(j + 1) * per] for j in range(pieces)]
        block = block[0] if pieces == 1 else jnp.concatenate(block, axis=1)
        logs.append(block[0:heads] + (block[heads:2 * heads] + block[2 * heads:3 * heads]))
    top = functools.reduce(jnp.maximum, logs)
    scales = [jnp.exp(l - top) for l in logs]
    total = functools.reduce(jnp.add, scales)
    turn_ref[...] = jnp.zeros_like(turn_ref)
    for i, scale in enumerate(scales):
        turn_ref[i * heads:(i + 1) * heads, :] = scale / total
    turned = turn_ref[...].T
    for h in range(heads):
        cols = slice(h * HEAD_SIZE, (h + 1) * HEAD_SIZE)
        acc = jnp.zeros((rows_all, HEAD_SIZE), f32)
        for i, part in enumerate(parts):
            at = i * heads + h
            acc = acc + turned[:, at:at + 1] * part[0:rows_all, cols].astype(f32)
        out[:, cols] = acc.astype(bf16)


def project_kernel(mine_ref, other_ref, w_mine_ref, w_other_ref, keep_ref, send_ref, *, outer, rows):
    me, z, r = place()
    y = lax.shift_right_logical(r, 1)

    def gather(ref, side):
        found = []
        for kk in range(outer):
            at = (lax.bitwise_xor(z, kk) * INNER + side * 2) * rows
            found.append(ref[pl.ds(pl.multiple_of(at, 2 * rows), 2 * rows), :])
        return jnp.concatenate(found, axis=0)

    for side, out in ((1 - y, send_ref), (y, keep_ref)):
        term = jnp.dot(gather(mine_ref, side), w_mine_ref[...], preferred_element_type=f32)
        term = term + jnp.dot(gather(other_ref, side), w_other_ref[...], preferred_element_type=f32)
        out[...] = term.astype(out.dtype)


def first_sum_kernel(keep_ref, got_ref, *out_refs, span):
    for kk, out in enumerate(out_refs):
        at = slice(kk * span, (kk + 1) * span)
        out[...] = (keep_ref[at, :] + got_ref[at, :].astype(f32)).astype(out.dtype)


def last_sum_kernel(*refs, rows):
    *parts, mine_ref, other_ref, total_ref = refs
    me, z, r = place()
    c = lax.bitwise_and(r, 1)
    total_ref[...] = functools.reduce(jnp.add, [p[...].astype(f32) for p in parts])
    mine_ref[...] = total_ref[pl.ds(pl.multiple_of(c * rows, rows), rows), :].astype(bf16)
    other_ref[...] = total_ref[pl.ds(pl.multiple_of((1 - c) * rows, rows), rows), :].astype(bf16)


def body(query_block, cache_keys, stored_values, live_counts, first_position, out_weight):
    devices = lax.axis_size("seq")
    outer = devices // INNER
    rows = query_block.shape[0]
    rows_all = rows * devices
    keys = cache_keys.shape[0]
    heads = QUERY_HEADS // devices
    width = heads * HEAD_SIZE
    copies = devices // KEY_VALUE_HEADS
    model = out_weight.shape[1]
    half = model // 2
    assert heads * copies == QUERY_HEADS // KEY_VALUE_HEADS and keys <= 256
    chunks = CHUNKS if half % (CHUNKS * 128) == 0 else 1
    cols = half // chunks
    me, z, r = place()
    c = lax.bitwise_and(r, 1)
    shape = jax.ShapeDtypeStruct

    def swap(x, k):
        return lax.ppermute(x, "seq", [(i, i ^ k) for i in range(devices)])

    q_out = call(
        functools.partial(split_queries_kernel, outer=outer, width=width),
        "split_queries", [query_block], [shape((outer, rows, width), bf16)] * INNER,
    )
    inner_q = jnp.stack([q_out[0]] + [swap(q_out[k], k) for k in range(1, INNER)])
    ys = [inner_q] + [swap(inner_q, k * INNER) for k in range(1, outer)]

    order = list(range(outer - 1, -1, -1))
    phases = [order[:outer // 2], order[outer // 2:]]
    partial_of = {}
    for offsets in phases:
        msgs = call(
            functools.partial(split_cache_kernel, offsets=offsets, copies=copies),
            "split_cache", [live_counts, cache_keys, stored_values],
            [shape((len(offsets), 2 * keys + 16, HEAD_SIZE), bf16)] * INNER, scalars=1,
        )
        kvs = [msgs[0]] + [swap(msgs[k], k) for k in range(1, INNER)]
        outs = call(
            functools.partial(
                attention_kernel, outer=outer, offsets=offsets, rows_all=rows_all, keys=keys,
                heads=heads, width=width,
            ),
            "attention", [first_position] + ys + kvs,
            [shape((rows_all + 16, width), bf16)] * len(offsets),
            scratch=[pltpu.VMEM((rows_all, INNER * keys), f32), pltpu.VMEM((rows_all, width), f32)],
            scalars=1,
            flops=4 * rows_all * INNER * keys * width * len(offsets),
        )
        for kk, out in zip(offsets, outs):
            partial_of[kk] = swap(out, kk * INNER) if kk else out

    (merged,) = call(
        functools.partial(merge_kernel, sources=outer, rows_all=rows_all, heads=heads, width=width),
        "merge", [partial_of[k] for k in range(outer)], [shape((rows_all, width), bf16)],
        scratch=[pltpu.VMEM((128, rows_all), f32)],
    )
    other = swap(merged, 1)

    w_mine = lax.dynamic_slice_in_dim(out_weight, c * half, half, 1)
    w_other = swap(lax.dynamic_slice_in_dim(out_weight, (1 - c) * half, half, 1), 1)

    span = 2 * rows
    mine_cols = []
    other_cols = []
    for j in range(chunks):
        at = slice(j * cols, (j + 1) * cols)
        keep, send = call(
            functools.partial(project_kernel, outer=outer, rows=rows),
            "project", [merged, other, w_mine[:, at], w_other[:, at]],
            [shape((outer * span, cols), f32), shape((outer * span, cols), bf16)],
            flops=4 * rows_all * width * cols,
        )
        got = swap(send, 2)
        sums = call(
            functools.partial(first_sum_kernel, span=span), "first_sum", [keep, got],
            [shape((span, cols), f32)] + [shape((span, cols), bf16)] * (outer - 1),
        )
        parts = [sums[0]] + [swap(sums[k], k * INNER) for k in range(1, outer)]
        mine, theirs = call(
            functools.partial(last_sum_kernel, rows=rows), "last_sum", parts,
            [shape((rows, cols), bf16)] * 2, scratch=[pltpu.VMEM((span, cols), f32)],
        )
        mine_cols.append(mine)
        other_cols.append(swap(theirs, 1))
    first = c == 0
    left = [jnp.where(first, a, b) for a, b in zip(mine_cols, other_cols)]
    right = [jnp.where(first, b, a) for a, b in zip(mine_cols, other_cols)]
    return jnp.concatenate(left + right, axis=1)


def solution(mesh):
    in_specs = (
        P(("groups", "seq"), None),
        P(("groups", "seq"), None),
        P(("groups", "seq"), None),
        P(("groups", "seq")),
        P("groups"),
        P("seq", None),
    )
    out_specs = P(("groups", "seq"), None)
    return jax.shard_map(body, mesh=mesh, in_specs=in_specs, out_specs=out_specs, check_vma=False)
```

```python
import functools

import jax
import jax.numpy as jnp
from jax import lax
from jax.experimental import pallas as pl
from jax.experimental.pallas import tpu as pltpu
from jax.sharding import PartitionSpec as P


QUERY_HEADS = 32
KEY_VALUE_HEADS = 16
HEAD_SIZE = 128
INNER = 4
CHUNKS = 3

score_scale = 168.0 ** (-0.5)
masked_value = -1e30
log2e = 1.4426950408889634
ln2 = 0.6931471805599453


bf16 = jnp.bfloat16
f32 = jnp.float32
VM = pltpu.MemorySpace.VMEM
SM = pltpu.MemorySpace.SMEM


def vspec():
    return pl.BlockSpec(memory_space=VM)


def sspec():
    return pl.BlockSpec(memory_space=SM)


def place():
    me = lax.axis_index("seq")
    return me, lax.shift_right_logical(me, 2), lax.bitwise_and(me, 3)


def call(kernel, ins, outs, scratch=(), scalars=0, flops=0):
    in_specs = [sspec()] * scalars + [vspec()] * (len(ins) - scalars)
    moved = sum(a.size * a.dtype.itemsize for a in list(ins) + list(outs))
    return pl.pallas_call(
        kernel,
        out_shape=tuple(outs),
        in_specs=in_specs,
        out_specs=tuple(vspec() for _ in outs),
        scratch_shapes=list(scratch),
        cost_estimate=pl.CostEstimate(flops=flops, transcendentals=0, bytes_accessed=moved),
    )(*ins)


def split_kernel(live_ref, q_ref, k_ref, v_ref, *refs, outer, width, groups, copies):
    _, z, r = place()
    q_outs = refs[:INNER]
    kv_outs = refs[INNER:INNER + len(groups)]
    live_rows, sems = refs[INNER + len(groups):]
    keys = k_ref.shape[0]
    started = []

    def copy(source, target):
        one = pltpu.make_async_copy(source, target, sems.at[len(started)])
        one.start()
        started.append(one)

    live_rows[...] = jnp.full(live_rows.shape, live_ref[0], jnp.int32).astype(f32).astype(bf16)
    for k, out in enumerate(q_outs):
        for zz in range(outer):
            col = pl.multiple_of((zz * INNER + lax.bitwise_xor(r, k)) * width, width)
            copy(q_ref.at[:, pl.ds(col, width)], out.at[zz])
    for (k, offsets), out in zip(groups, kv_outs):
        for i, kk in enumerate(offsets):
            head = lax.bitwise_xor(z, kk) * INNER + lax.bitwise_xor(r, k)
            col = pl.multiple_of((head // copies) * HEAD_SIZE, HEAD_SIZE)
            copy(k_ref.at[:, pl.ds(col, HEAD_SIZE)], out.at[i, pl.ds(0, keys), :])
            copy(v_ref.at[:, pl.ds(col, HEAD_SIZE)], out.at[i, pl.ds(keys, keys), :])
            copy(live_rows, out.at[i, pl.ds(2 * keys, 16), :])
    for one in started:
        one.wait()


def split_weight_kernel(w_ref, out_ref, sem):
    _, _, r = place()
    half = out_ref.shape[1]
    col = pl.multiple_of((1 - lax.bitwise_and(r, 1)) * half, 128)
    one = pltpu.make_async_copy(w_ref.at[:, pl.ds(col, half)], out_ref, sem)
    one.start()
    one.wait()


def attention_kernel(first_ref, *refs, outer, offsets, rows_all, keys, heads, width):
    ys = refs[:outer]
    kvs = refs[outer:outer + INNER]
    outs = refs[outer + INNER:outer + INNER + len(offsets)]
    bias_ref, q_ref = refs[outer + INNER + len(offsets):]
    _, z, r = place()
    rows = rows_all // (outer * INNER)
    q_pos = first_ref[0] + lax.broadcasted_iota(jnp.int32, (rows_all, keys), 0)
    lane = lax.broadcasted_iota(jnp.int32, (rows_all, keys), 1)
    lane_f = lane.astype(f32)
    for k in range(INNER):
        start = (z * INNER + lax.bitwise_xor(r, k)) * keys
        live = kvs[k][0, 2 * keys:2 * keys + 1, :].astype(f32)
        live = jnp.concatenate([live] * (keys // HEAD_SIZE), axis=1)
        allowed = (lane_f < live) & (start + lane <= q_pos)
        bias_ref[:, k * keys:(k + 1) * keys] = jnp.where(allowed, 0.0, masked_value)
    column = lax.broadcasted_iota(jnp.int32, (rows_all, 128), 1)
    for i, kk in enumerate(offsets):
        zz = lax.bitwise_xor(z, kk)
        for k2 in range(outer):
            for k in range(INNER):
                src = lax.bitwise_xor(z, k2) * INNER + lax.bitwise_xor(r, k)
                at = pl.multiple_of(src * rows, rows)
                q_ref[pl.ds(at, rows), :] = ys[k2][k, zz].astype(f32)
        stats = jnp.zeros((rows_all, 128), f32)
        for h in range(heads):
            cols = slice(h * HEAD_SIZE, (h + 1) * HEAD_SIZE)
            query = q_ref[:, cols].astype(bf16)
            scores = []
            for k in range(INNER):
                part = lax.dot_general(
                    query, kvs[k][i, 0:keys, :], (((1,), (1,)), ((), ())),
                    preferred_element_type=f32,
                )
                scores.append(part * (score_scale * log2e) + bias_ref[:, k * keys:(k + 1) * keys])
            top = functools.reduce(jnp.maximum, scores)
            best = jnp.maximum(jnp.max(top, axis=1, keepdims=True), -1e29)
            acc = jnp.zeros((rows_all, HEAD_SIZE), f32)
            sums = jnp.zeros((rows_all, keys), f32)
            for k in range(INNER):
                weights = jnp.exp2(scores[k] - best)
                sums = sums + weights
                acc = acc + jnp.dot(
                    weights.astype(bf16), kvs[k][i, keys:2 * keys, :], preferred_element_type=f32
                )
            total = jnp.sum(sums, axis=1, keepdims=True)
            safe = jnp.where(total > 0, total, 1.0)
            outs[i][0:rows_all, cols] = (acc / safe).astype(bf16)
            logsum = jnp.where(total > 0, best * ln2 + jnp.log(safe), masked_value)
            high = logsum.astype(bf16).astype(f32)
            rest = logsum - high
            mid = rest.astype(bf16).astype(f32)
            low = rest - mid
            for p, piece in enumerate((high, mid, low)):
                stats = jnp.where(column == p * heads + h, piece, stats)
        turned = stats.T
        pieces = rows_all // width
        per = 16 // pieces
        block = [turned[0:per, j * width:(j + 1) * width] for j in range(pieces)]
        block = block[0] if pieces == 1 else jnp.concatenate(block, axis=0)
        outs[i][rows_all:rows_all + 16, :] = block.astype(bf16)


def merge_kernel(*refs, sources, rows_all, heads, width):
    parts = refs[:sources]
    out, turn_ref = refs[sources:]
    pieces = rows_all // width
    per = 16 // pieces
    logs = []
    for part in parts:
        block = part[rows_all:rows_all + 16, :].astype(f32)
        block = [block[j * per:(j + 1) * per] for j in range(pieces)]
        block = block[0] if pieces == 1 else jnp.concatenate(block, axis=1)
        logs.append(block[0:heads] + (block[heads:2 * heads] + block[2 * heads:3 * heads]))
    top = functools.reduce(jnp.maximum, logs)
    scales = [jnp.exp(l - top) for l in logs]
    total = functools.reduce(jnp.add, scales)
    turn_ref[...] = jnp.zeros_like(turn_ref)
    for i, scale in enumerate(scales):
        turn_ref[i * heads:(i + 1) * heads, :] = scale / total
    turned = turn_ref[...].T
    for h in range(heads):
        cols = slice(h * HEAD_SIZE, (h + 1) * HEAD_SIZE)
        acc = jnp.zeros((rows_all, HEAD_SIZE), f32)
        for i, part in enumerate(parts):
            at = i * heads + h
            acc = acc + turned[:, at:at + 1] * part[0:rows_all, cols].astype(f32)
        out[:, cols] = acc.astype(bf16)


def project_kernel(side_ref, mine_ref, other_ref, w_mine_ref, w_other_ref, *out_refs, groups, rows):
    _, z, r = place()
    y = lax.shift_right_logical(r, 1)

    def gather(ref, side):
        found = []
        for group in groups:
            for kk in group:
                at = (lax.bitwise_xor(z, kk) * INNER + side * 2) * rows
                found.append(ref[pl.ds(pl.multiple_of(at, 2 * rows), 2 * rows), :])
        return jnp.concatenate(found, axis=0)

    for side, outs in ((1 - y, out_refs[:len(groups)]), (y, out_refs[len(groups):])):
        term = jnp.dot(gather(mine_ref, side), w_mine_ref[...], preferred_element_type=f32)
        term = term + jnp.dot(gather(other_ref, side), w_other_ref[...], preferred_element_type=f32)
        at = 0
        for group, out in zip(groups, outs):
            size = 2 * rows * len(group)
            out[...] = term[at:at + size].astype(out.dtype)
            at += size


def first_sum_kernel(keep_ref, got_ref, *out_refs, span):
    for i, out in enumerate(out_refs):
        at = slice(i * span, (i + 1) * span)
        out[...] = (keep_ref[at, :] + got_ref[at, :].astype(f32)).astype(out.dtype)


def last_sum_kernel(keep_ref, got_ref, *refs, rows):
    *parts, mine_ref, other_ref, total_ref = refs
    _, _, r = place()
    c = lax.bitwise_and(r, 1)
    total = keep_ref[...] + got_ref[...].astype(f32)
    for part in parts:
        total = total + part[...].astype(f32)
    total_ref[...] = total
    mine_ref[...] = total_ref[pl.ds(pl.multiple_of(c * rows, rows), rows), :].astype(bf16)
    other_ref[...] = total_ref[pl.ds(pl.multiple_of((1 - c) * rows, rows), rows), :].astype(bf16)


def join_kernel(mine_ref, other_ref, out_ref):
    _, _, r = place()
    c = lax.bitwise_and(r, 1)
    half = mine_ref.shape[1]
    out_ref[:, pl.ds(pl.multiple_of(c * half, 128), half)] = mine_ref[...]
    out_ref[:, pl.ds(pl.multiple_of((1 - c) * half, 128), half)] = other_ref[...]


def layer(query_block, cache_keys, stored_values, live_counts, first_position, out_weight):
    devices = lax.axis_size("seq")
    outer = devices // INNER
    rows = query_block.shape[0]
    rows_all = rows * devices
    keys = cache_keys.shape[0]
    heads = QUERY_HEADS // devices
    width = heads * HEAD_SIZE
    copies = devices // KEY_VALUE_HEADS
    model = out_weight.shape[1]
    half = model // 2
    assert heads * copies == QUERY_HEADS // KEY_VALUE_HEADS and keys <= 256
    blocks = CHUNKS if half % (CHUNKS * 128) == 0 else 1
    cols = half // blocks
    shape = jax.ShapeDtypeStruct
    anywhere = pl.BlockSpec(memory_space=pl.ANY)

    def swap(x, k):
        return lax.ppermute(x, "seq", [(i, i ^ k) for i in range(devices)])

    order = list(range(outer - 1, -1, -1))
    phases = [order[:outer // 2], order[outer // 2:3 * outer // 4], order[3 * outer // 4:]]
    groups = [(0, order), (1, order)] + [(k, p) for p in phases for k in range(2, INNER)]
    outs = [shape((outer, rows, width), bf16)] * INNER + [
        shape((len(p), 2 * keys + 16, HEAD_SIZE), bf16) for k, p in groups
    ]
    copies_started = INNER * outer + sum(3 * len(p) for k, p in groups)
    split = pl.pallas_call(
        functools.partial(
            split_kernel, outer=outer, width=width, groups=groups, copies=copies
        ),
        out_shape=tuple(outs),
        in_specs=[sspec(), anywhere, anywhere, anywhere],
        out_specs=tuple(anywhere for _ in outs),
        scratch_shapes=[
            pltpu.VMEM((16, HEAD_SIZE), bf16), pltpu.SemaphoreType.DMA((copies_started,)),
        ],
        name="split",
    )(live_counts, query_block, cache_keys, stored_values)
    q_out, kv_out = split[:INNER], split[INNER:]
    q_got = {k: swap(q_out[k], k) for k in (2, 3, 1)}
    kv_pair = swap(kv_out[1], 1)
    kv_far = [
        {k: swap(kv_out[2 + 2 * i + k - 2], k) for k in range(2, INNER)}
        for i in range(len(phases))
    ]
    inner_q = jnp.stack([q_out[0], q_got[1], q_got[2], q_got[3]])
    ys = [inner_q] + [swap(inner_q, k * INNER) for k in range(1, outer)]

    w_send = pl.pallas_call(
        split_weight_kernel,
        out_shape=shape((out_weight.shape[0], half), bf16),
        in_specs=[anywhere],
        out_specs=anywhere,
        scratch_shapes=[pltpu.SemaphoreType.DMA],
        name="split_weight",
    )(out_weight)
    w_other = swap(w_send, 1)

    partial_of = {}
    at = 0
    for i, offsets in enumerate(phases):
        size = len(offsets)
        near = pl.BlockSpec(
            (size, 2 * keys + 16, HEAD_SIZE), functools.partial(lambda b, g: (b, 0, 0), at // size)
        )
        outs = pl.pallas_call(
            functools.partial(
                attention_kernel, outer=outer, offsets=offsets, rows_all=rows_all, keys=keys,
                heads=heads, width=width,
            ),
            out_shape=tuple([shape((rows_all + 16, width), bf16)] * size),
            grid=(1,),
            in_specs=[sspec()] + [vspec()] * outer + [near, near] + [vspec()] * (INNER - 2),
            out_specs=tuple(vspec() for _ in offsets),
            scratch_shapes=[
                pltpu.VMEM((rows_all, INNER * keys), f32), pltpu.VMEM((rows_all, width), f32),
            ],
            name="attention",
            cost_estimate=pl.CostEstimate(
                flops=4 * rows_all * INNER * keys * width * size, transcendentals=0,
                bytes_accessed=2 * INNER * keys * HEAD_SIZE * 2 * size,
            ),
        )(first_position, *ys, kv_out[0], kv_pair, kv_far[i][2], kv_far[i][3])
        at += size
        for kk, out in zip(offsets, outs):
            partial_of[kk] = swap(out, kk * INNER) if kk else out

    (merged,) = call(
        functools.partial(merge_kernel, sources=outer, rows_all=rows_all, heads=heads, width=width),
        [partial_of[k] for k in range(outer)], [shape((rows_all, width), bf16)],
        scratch=[pltpu.VMEM((128, rows_all), f32)],
    )
    other = swap(merged, 1)

    span = 2 * rows
    term_groups = [[kk] for kk in order[:-2]] + [order[-2:]]
    side = lax.bitwise_and(lax.axis_index("seq"), 1).reshape(1)
    out_shapes = [shape((span * len(g), half), bf16) for g in term_groups]
    out_shapes += [shape((span * len(g), half), f32) for g in term_groups]
    terms = pl.pallas_call(
        functools.partial(project_kernel, groups=term_groups, rows=rows),
        out_shape=tuple(out_shapes),
        grid_spec=pltpu.PrefetchScalarGridSpec(
            num_scalar_prefetch=1,
            grid=(blocks,),
            in_specs=[
                pl.BlockSpec((rows_all, width), lambda j, side: (0, 0)),
                pl.BlockSpec((rows_all, width), lambda j, side: (0, 0)),
                pl.BlockSpec((width, cols), lambda j, side: (0, side[0] * blocks + j)),
                pl.BlockSpec((width, cols), lambda j, side: (0, j)),
            ],
            out_specs=tuple(
                pl.BlockSpec((o.shape[0], cols), lambda j, side: (0, j)) for o in out_shapes
            ),
        ),
        name="project",
        cost_estimate=pl.CostEstimate(
            flops=4 * rows_all * width * half, transcendentals=0,
            bytes_accessed=4 * width * half,
        ),
    )(side, merged, other, out_weight, w_other)
    sends, keeps = terms[:len(term_groups)], terms[len(term_groups):]
    gots = [swap(x, 2) for x in sends]
    parts = []
    for i, group in enumerate(term_groups):
        moved = [kk for kk in group if kk]
        keep, got = keeps[i], gots[i]
        sums = pl.pallas_call(
            functools.partial(first_sum_kernel, span=span),
            out_shape=tuple([shape((span, half), bf16)] * len(moved)),
            grid=(1,),
            in_specs=[pl.BlockSpec((span * len(moved), half), lambda g: (0, 0))] * 2,
            out_specs=tuple(vspec() for _ in moved),
            name="first_sum",
        )(keep, got)
        parts += [swap(x, kk * INNER) for kk, x in zip(moved, sums)]
    last = len(term_groups[-1]) - 1
    mine, theirs = pl.pallas_call(
        functools.partial(last_sum_kernel, rows=rows),
        out_shape=tuple([shape((rows, half), bf16)] * 2),
        grid=(1,),
        in_specs=[pl.BlockSpec((span, half), lambda g: (last, 0))] * 2 + [vspec()] * len(parts),
        out_specs=(vspec(), vspec()),
        scratch_shapes=[pltpu.VMEM((span, half), f32)],
        name="last_sum",
    )(keeps[-1], gots[-1], *parts)
    (joined,) = call(join_kernel, [mine, swap(theirs, 1)], [shape((rows, model), bf16)])
    return joined


def solution(mesh):
    in_specs = (
        P(("groups", "seq"), None),
        P(("groups", "seq"), None),
        P(("groups", "seq"), None),
        P(("groups", "seq")),
        P("groups"),
        P("seq", None),
    )
    out_specs = P(("groups", "seq"), None)
    return jax.shard_map(layer, mesh=mesh, in_specs=in_specs, out_specs=out_specs, check_vma=False)
```

```python
import functools

import jax
import jax.numpy as jnp
from jax import lax
from jax.experimental import pallas as pl
from jax.experimental.pallas import tpu as pltpu
from jax.sharding import PartitionSpec as P


QUERY_HEADS = 32
KEY_VALUE_HEADS = 16
HEAD_SIZE = 128
INNER = 4
CHUNKS = 3

score_scale = 168.0 ** (-0.5)
masked_value = -1e30
log2e = 1.4426950408889634
ln2 = 0.6931471805599453


bf16 = jnp.bfloat16
f32 = jnp.float32
VM = pltpu.MemorySpace.VMEM
SM = pltpu.MemorySpace.SMEM


def vspec():
    return pl.BlockSpec(memory_space=VM)


def sspec():
    return pl.BlockSpec(memory_space=SM)


def place():
    me = lax.axis_index("seq")
    return me, lax.shift_right_logical(me, 2), lax.bitwise_and(me, 3)


def call(kernel, ins, outs, scratch=(), scalars=0, flops=0, limit=8):
    in_specs = [sspec()] * scalars + [vspec()] * (len(ins) - scalars)
    moved = sum(a.size * a.dtype.itemsize for a in list(ins) + list(outs))
    return pl.pallas_call(
        kernel,
        out_shape=tuple(outs),
        in_specs=in_specs,
        out_specs=tuple(vspec() for _ in outs),
        scratch_shapes=list(scratch),
        cost_estimate=pl.CostEstimate(flops=flops, transcendentals=0, bytes_accessed=moved),
        compiler_params=pltpu.CompilerParams(vmem_limit_bytes=limit << 20),
    )(*ins)


def split_kernel(live_ref, q_ref, k_ref, v_ref, *refs, outer, width, groups, copies):
    _, z, r = place()
    q_outs = refs[:INNER]
    kv_outs = refs[INNER:]
    keys = k_ref.shape[0]
    live = jnp.full((16, HEAD_SIZE), live_ref[0], jnp.int32).astype(f32).astype(bf16)
    for k, out in enumerate(q_outs):
        for zz in range(outer):
            col = pl.multiple_of((zz * INNER + lax.bitwise_xor(r, k)) * width, width)
            out[zz] = q_ref[:, pl.ds(col, width)]
    for (k, offsets), out in zip(groups, kv_outs):
        for i, kk in enumerate(offsets):
            head = lax.bitwise_xor(z, kk) * INNER + lax.bitwise_xor(r, k)
            col = pl.multiple_of((head // copies) * HEAD_SIZE, HEAD_SIZE)
            out[i, 0:keys, :] = k_ref[:, pl.ds(col, HEAD_SIZE)]
            out[i, keys:2 * keys, :] = v_ref[:, pl.ds(col, HEAD_SIZE)]
            out[i, 2 * keys:2 * keys + 16, :] = live


def split_weight_kernel(w_ref, out_ref):
    _, _, r = place()
    half = out_ref.shape[1]
    col = pl.multiple_of((1 - lax.bitwise_and(r, 1)) * half, 128)
    out_ref[...] = w_ref[:, pl.ds(col, half)]


def attention_kernel(first_ref, *refs, outer, first, offsets, rows_all, keys, heads, width):
    ys = refs[:outer]
    kvs = refs[outer:outer + INNER]
    begin = [first, first] + [0] * (INNER - 2)
    outs = refs[outer + INNER:outer + INNER + len(offsets)]
    bias_ref, q_ref = refs[outer + INNER + len(offsets):]
    _, z, r = place()
    rows = rows_all // (outer * INNER)
    q_pos = first_ref[0] + lax.broadcasted_iota(jnp.int32, (rows_all, keys), 0)
    lane = lax.broadcasted_iota(jnp.int32, (rows_all, keys), 1)
    lane_f = lane.astype(f32)
    for k in range(INNER):
        start = (z * INNER + lax.bitwise_xor(r, k)) * keys
        live = kvs[k][0, 2 * keys:2 * keys + 1, :].astype(f32)
        live = jnp.concatenate([live] * (keys // HEAD_SIZE), axis=1)
        allowed = (lane_f < live) & (start + lane <= q_pos)
        bias_ref[:, k * keys:(k + 1) * keys] = jnp.where(allowed, 0.0, masked_value)
    column = lax.broadcasted_iota(jnp.int32, (rows_all, 128), 1)
    for i, kk in enumerate(offsets):
        zz = lax.bitwise_xor(z, kk)
        for k2 in range(outer):
            for k in range(INNER):
                src = lax.bitwise_xor(z, k2) * INNER + lax.bitwise_xor(r, k)
                at = pl.multiple_of(src * rows, rows)
                q_ref[pl.ds(at, rows), :] = ys[k2][k, zz].astype(f32)
        stats = jnp.zeros((rows_all, 128), f32)
        for h in range(heads):
            cols = slice(h * HEAD_SIZE, (h + 1) * HEAD_SIZE)
            query = q_ref[:, cols].astype(bf16)
            scores = []
            for k in range(INNER):
                part = lax.dot_general(
                    query, kvs[k][begin[k] + i, 0:keys, :], (((1,), (1,)), ((), ())),
                    preferred_element_type=f32,
                )
                scores.append(part * (score_scale * log2e) + bias_ref[:, k * keys:(k + 1) * keys])
            top = functools.reduce(jnp.maximum, scores)
            best = jnp.maximum(jnp.max(top, axis=1, keepdims=True), -1e29)
            acc = jnp.zeros((rows_all, HEAD_SIZE), f32)
            sums = jnp.zeros((rows_all, keys), f32)
            for k in range(INNER):
                weights = jnp.exp2(scores[k] - best)
                sums = sums + weights
                acc = acc + jnp.dot(
                    weights.astype(bf16), kvs[k][begin[k] + i, keys:2 * keys, :], preferred_element_type=f32
                )
            total = jnp.sum(sums, axis=1, keepdims=True)
            safe = jnp.where(total > 0, total, 1.0)
            outs[i][0:rows_all, cols] = (acc / safe).astype(bf16)
            logsum = jnp.where(total > 0, best * ln2 + jnp.log(safe), masked_value)
            high = logsum.astype(bf16).astype(f32)
            rest = logsum - high
            mid = rest.astype(bf16).astype(f32)
            low = rest - mid
            for p, piece in enumerate((high, mid, low)):
                stats = jnp.where(column == p * heads + h, piece, stats)
        turned = stats.T
        pieces = rows_all // width
        per = 16 // pieces
        block = [turned[0:per, j * width:(j + 1) * width] for j in range(pieces)]
        block = block[0] if pieces == 1 else jnp.concatenate(block, axis=0)
        outs[i][rows_all:rows_all + 16, :] = block.astype(bf16)


def merge_kernel(*refs, sources, rows_all, heads, width):
    parts = refs[:sources]
    out, turn_ref = refs[sources:]
    pieces = rows_all // width
    per = 16 // pieces
    logs = []
    for part in parts:
        block = part[rows_all:rows_all + 16, :].astype(f32)
        block = [block[j * per:(j + 1) * per] for j in range(pieces)]
        block = block[0] if pieces == 1 else jnp.concatenate(block, axis=1)
        logs.append(block[0:heads] + (block[heads:2 * heads] + block[2 * heads:3 * heads]))
    top = functools.reduce(jnp.maximum, logs)
    scales = [jnp.exp(l - top) for l in logs]
    total = functools.reduce(jnp.add, scales)
    turn_ref[...] = jnp.zeros_like(turn_ref)
    for i, scale in enumerate(scales):
        turn_ref[i * heads:(i + 1) * heads, :] = scale / total
    turned = turn_ref[...].T
    for h in range(heads):
        cols = slice(h * HEAD_SIZE, (h + 1) * HEAD_SIZE)
        acc = jnp.zeros((rows_all, HEAD_SIZE), f32)
        for i, part in enumerate(parts):
            at = i * heads + h
            acc = acc + turned[:, at:at + 1] * part[0:rows_all, cols].astype(f32)
        out[:, cols] = acc.astype(bf16)


def project_kernel(mine_ref, other_ref, w_mine_ref, w_other_ref, *out_refs, groups, rows, blocks):
    _, z, r = place()
    y = lax.shift_right_logical(r, 1)
    half = w_other_ref.shape[1]
    cols = half // blocks

    def gather(ref, side):
        found = []
        for group in groups:
            for kk in group:
                at = (lax.bitwise_xor(z, kk) * INNER + side * 2) * rows
                found.append(ref[pl.ds(pl.multiple_of(at, 2 * rows), 2 * rows), :])
        return jnp.concatenate(found, axis=0)

    mine = jnp.concatenate([gather(mine_ref, 1 - y), gather(mine_ref, y)], axis=0)
    other = jnp.concatenate([gather(other_ref, 1 - y), gather(other_ref, y)], axis=0)
    for j in range(blocks):
        here = slice(j * cols, (j + 1) * cols)
        col = pl.multiple_of(lax.bitwise_and(r, 1) * half + j * cols, 128)
        term = jnp.dot(mine, w_mine_ref[:, pl.ds(col, cols)], preferred_element_type=f32)
        term = term + jnp.dot(other, w_other_ref[:, here], preferred_element_type=f32)
        at = 0
        for group, out in zip(groups + groups, out_refs):
            size = 2 * rows * len(group)
            out[:, here] = term[at:at + size].astype(out.dtype)
            at += size


def first_sum_kernel(keep_ref, got_ref, out_ref):
    out_ref[...] = (keep_ref[...] + got_ref[...].astype(f32)).astype(out_ref.dtype)


def last_sum_kernel(keep_ref, got_ref, *refs, rows):
    *parts, mine_ref, other_ref, total_ref = refs
    _, _, r = place()
    c = lax.bitwise_and(r, 1)
    total = keep_ref[...] + got_ref[...].astype(f32)
    for part in parts:
        total = total + part[...].astype(f32)
    total_ref[...] = total
    mine_ref[...] = total_ref[pl.ds(pl.multiple_of(c * rows, rows), rows), :].astype(bf16)
    other_ref[...] = total_ref[pl.ds(pl.multiple_of((1 - c) * rows, rows), rows), :].astype(bf16)


def join_kernel(mine_ref, other_ref, out_ref):
    _, _, r = place()
    c = lax.bitwise_and(r, 1)
    half = mine_ref.shape[1]
    out_ref[:, pl.ds(pl.multiple_of(c * half, 128), half)] = mine_ref[...]
    out_ref[:, pl.ds(pl.multiple_of((1 - c) * half, 128), half)] = other_ref[...]


def layer(query_block, cache_keys, stored_values, live_counts, first_position, out_weight):
    devices = lax.axis_size("seq")
    outer = devices // INNER
    rows = query_block.shape[0]
    rows_all = rows * devices
    keys = cache_keys.shape[0]
    heads = QUERY_HEADS // devices
    width = heads * HEAD_SIZE
    copies = devices // KEY_VALUE_HEADS
    model = out_weight.shape[1]
    half = model // 2
    assert heads * copies == QUERY_HEADS // KEY_VALUE_HEADS and keys <= 256
    blocks = CHUNKS if half % (CHUNKS * 128) == 0 else 1
    shape = jax.ShapeDtypeStruct

    def swap(x, k):
        return lax.ppermute(x, "seq", [(i, i ^ k) for i in range(devices)])

    order = list(range(outer - 1, -1, -1))
    phases = [order[:outer // 2], order[outer // 2:3 * outer // 4], order[3 * outer // 4:]]
    groups = [(0, order), (1, order)] + [(k, p) for p in phases for k in range(2, INNER)]
    outs = [shape((outer, rows, width), bf16)] * INNER + [
        shape((len(p), 2 * keys + 16, HEAD_SIZE), bf16) for k, p in groups
    ]
    split = call(
        functools.partial(split_kernel, outer=outer, width=width, groups=groups, copies=copies),
        [live_counts, query_block, cache_keys, stored_values], outs, scalars=1,
    )
    q_out, kv_out = split[:INNER], split[INNER:]
    q_got = {k: swap(q_out[k], k) for k in (2, 3, 1)}
    kv_pair = swap(kv_out[1], 1)
    kv_far = [
        {k: swap(kv_out[2 + 2 * i + k - 2], k) for k in range(2, INNER)}
        for i in range(len(phases))
    ]
    inner_q = jnp.stack([q_out[0], q_got[1], q_got[2], q_got[3]])
    ys = [inner_q] + [swap(inner_q, k * INNER) for k in range(1, outer)]

    (w_send,) = call(
        split_weight_kernel, [out_weight],
        [shape((out_weight.shape[0], half), bf16)],
    )
    w_other = swap(w_send, 1)

    partial_of = {}
    at = 0
    for i, offsets in enumerate(phases):
        size = len(offsets)
        outs = call(
            functools.partial(
                attention_kernel, outer=outer, first=at, offsets=offsets, rows_all=rows_all,
                keys=keys, heads=heads, width=width,
            ),
            [first_position, *ys, kv_out[0], kv_pair, kv_far[i][2], kv_far[i][3]],
            [shape((rows_all + 16, width), bf16)] * size,
            scratch=[pltpu.VMEM((rows_all, INNER * keys), f32), pltpu.VMEM((rows_all, width), f32)],
            scalars=1, flops=4 * rows_all * INNER * keys * width * size, limit=20,
        )
        at += size
        for kk, out in zip(offsets, outs):
            partial_of[kk] = swap(out, kk * INNER) if kk else out

    (merged,) = call(
        functools.partial(merge_kernel, sources=outer, rows_all=rows_all, heads=heads, width=width),
        [partial_of[k] for k in range(outer)], [shape((rows_all, width), bf16)],
        scratch=[pltpu.VMEM((128, rows_all), f32)],
    )
    other = swap(merged, 1)

    span = 2 * rows
    term_groups = [[kk] for kk in order]
    terms = call(
        functools.partial(project_kernel, groups=term_groups, rows=rows, blocks=blocks),
        [merged, other, out_weight, w_other],
        [shape((span * len(g), half), bf16) for g in term_groups]
        + [shape((span * len(g), half), f32) for g in term_groups],
        flops=4 * rows_all * width * half, limit=20,
    )
    sends, keeps = terms[:outer], terms[outer:]
    gots = [swap(x, 2) for x in sends]
    parts = []
    for i, kk in enumerate(order[:-1]):
        (part,) = call(first_sum_kernel, [keeps[i], gots[i]], [shape((span, half), bf16)])
        parts.append(swap(part, kk * INNER))
    mine, theirs = call(
        functools.partial(last_sum_kernel, rows=rows), [keeps[-1], gots[-1]] + parts,
        [shape((rows, half), bf16)] * 2, scratch=[pltpu.VMEM((span, half), f32)],
    )
    (joined,) = call(join_kernel, [mine, swap(theirs, 1)], [shape((rows, model), bf16)])
    return joined


def solution(mesh):
    in_specs = (
        P(("groups", "seq"), None),
        P(("groups", "seq"), None),
        P(("groups", "seq"), None),
        P(("groups", "seq")),
        P("groups"),
        P("seq", None),
    )
    out_specs = P(("groups", "seq"), None)
    return jax.shard_map(layer, mesh=mesh, in_specs=in_specs, out_specs=out_specs, check_vma=False)
```

```python
import functools

import jax
import jax.numpy as jnp
from jax import lax
from jax.experimental import pallas as pl
from jax.experimental.pallas import tpu as pltpu
from jax.sharding import PartitionSpec as P


QUERY_HEADS = 32
KEY_VALUE_HEADS = 16
HEAD_SIZE = 128
INNER = 4
SIDES = INNER // 2
CHUNKS = 3

score_scale = 168.0 ** (-0.5)
masked_value = -1e30
log2e = 1.4426950408889634
ln2 = 0.6931471805599453


bf16 = jnp.bfloat16
f32 = jnp.float32
VM = pltpu.MemorySpace.VMEM
SM = pltpu.MemorySpace.SMEM


def vspec():
    return pl.BlockSpec(memory_space=VM)


def sspec():
    return pl.BlockSpec(memory_space=SM)


def place():
    me = lax.axis_index("seq")
    return me, lax.shift_right_logical(me, 2), lax.bitwise_and(me, 3)


def call(kernel, ins, outs, scratch=(), scalars=0, flops=0, limit=8):
    in_specs = [sspec()] * scalars + [vspec()] * (len(ins) - scalars)
    moved = sum(a.size * a.dtype.itemsize for a in list(ins) + list(outs))
    return pl.pallas_call(
        kernel,
        out_shape=tuple(outs),
        in_specs=in_specs,
        out_specs=tuple(vspec() for _ in outs),
        scratch_shapes=list(scratch),
        cost_estimate=pl.CostEstimate(flops=flops, transcendentals=0, bytes_accessed=moved),
        compiler_params=pltpu.CompilerParams(vmem_limit_bytes=limit << 20),
    )(*ins)


def split_kernel(live_ref, q_hbm, k_hbm, v_hbm, *refs, outer, width, groups, copies):
    _, z, r = place()
    pair_out = refs[0]
    q_outs = refs[1:1 + SIDES]
    kv_outs = refs[1 + SIDES:1 + SIDES + len(groups)]
    q_ref, k_ref, v_ref, sems = refs[1 + SIDES + len(groups):]
    loads = [
        pltpu.make_async_copy(source, target, sems.at[i])
        for i, (source, target) in enumerate(((q_hbm, q_ref), (k_hbm, k_ref), (v_hbm, v_ref)))
    ]
    for load in loads:
        load.start()
    keys = k_ref.shape[0]
    live = jnp.full((16, HEAD_SIZE), live_ref[0], jnp.int32).astype(f32).astype(bf16)
    loads[0].wait()
    for j in range(SIDES):
        for zz in range(outer):
            for k in range(2):
                group = zz * INNER + lax.bitwise_xor(r, 2 * j + k)
                piece = q_ref[:, pl.ds(pl.multiple_of(group * width, width), width)]
                if k:
                    pair_out[j, zz] = piece
                else:
                    q_outs[j][zz] = piece
    loads[1].wait()
    loads[2].wait()
    for (k, offsets), out in zip(groups, kv_outs):
        for i, kk in enumerate(offsets):
            head = lax.bitwise_xor(z, kk) * INNER + lax.bitwise_xor(r, k)
            col = pl.multiple_of((head // copies) * HEAD_SIZE, HEAD_SIZE)
            out[i, 0:keys, :] = k_ref[:, pl.ds(col, HEAD_SIZE)]
            out[i, keys:2 * keys, :] = v_ref[:, pl.ds(col, HEAD_SIZE)]
            out[i, 2 * keys:2 * keys + 16, :] = live


def split_weight_kernel(w_ref, out_ref):
    _, _, r = place()
    half = out_ref.shape[1]
    col = pl.multiple_of((1 - lax.bitwise_and(r, 1)) * half, 128)
    out_ref[...] = w_ref[:, pl.ds(col, half)]


def attention_kernel(first_ref, *refs, outer, begin, offsets, rows_all, keys, heads, width):
    pieces = outer * SIDES
    ys = refs[:pieces]
    kvs = refs[pieces:pieces + INNER]
    outs = refs[pieces + INNER:pieces + INNER + len(offsets)]
    bias_ref, q_ref = refs[pieces + INNER + len(offsets):]
    _, z, r = place()
    rows = rows_all // (outer * INNER)
    q_pos = first_ref[0] + lax.broadcasted_iota(jnp.int32, (rows_all, keys), 0)
    lane = lax.broadcasted_iota(jnp.int32, (rows_all, keys), 1)
    lane_f = lane.astype(f32)
    for k in range(INNER):
        start = (z * INNER + lax.bitwise_xor(r, k)) * keys
        live = kvs[k][0, 2 * keys:2 * keys + 1, :].astype(f32)
        live = jnp.concatenate([live] * (keys // HEAD_SIZE), axis=1)
        allowed = (lane_f < live) & (start + lane <= q_pos)
        bias_ref[:, k * keys:(k + 1) * keys] = jnp.where(allowed, 0.0, masked_value)
    column = lax.broadcasted_iota(jnp.int32, (rows_all, 128), 1)
    for i, kk in enumerate(offsets):
        zz = lax.bitwise_xor(z, kk)
        for k2 in range(outer):
            for k in range(INNER):
                src = lax.bitwise_xor(z, k2) * INNER + lax.bitwise_xor(r, k)
                at = pl.multiple_of(src * rows, rows)
                q_ref[pl.ds(at, rows), :] = ys[k2 * SIDES + k // 2][k % 2, zz].astype(f32)
        stats = jnp.zeros((rows_all, 128), f32)
        for h in range(heads):
            cols = slice(h * HEAD_SIZE, (h + 1) * HEAD_SIZE)
            query = q_ref[:, cols].astype(bf16)
            scores = []
            for k in range(INNER):
                part = lax.dot_general(
                    query, kvs[k][begin[k] + i, 0:keys, :], (((1,), (1,)), ((), ())),
                    preferred_element_type=f32,
                )
                scores.append(part * (score_scale * log2e) + bias_ref[:, k * keys:(k + 1) * keys])
            top = functools.reduce(jnp.maximum, scores)
            best = jnp.maximum(jnp.max(top, axis=1, keepdims=True), -1e29)
            acc = jnp.zeros((rows_all, HEAD_SIZE), f32)
            sums = jnp.zeros((rows_all, keys), f32)
            for k in range(INNER):
                weights = jnp.exp2(scores[k] - best)
                sums = sums + weights
                acc = acc + jnp.dot(
                    weights.astype(bf16), kvs[k][begin[k] + i, keys:2 * keys, :], preferred_element_type=f32
                )
            total = jnp.sum(sums, axis=1, keepdims=True)
            safe = jnp.where(total > 0, total, 1.0)
            outs[i][0:rows_all, cols] = (acc / safe).astype(bf16)
            logsum = jnp.where(total > 0, best * ln2 + jnp.log(safe), masked_value)
            high = logsum.astype(bf16).astype(f32)
            rest = logsum - high
            mid = rest.astype(bf16).astype(f32)
            low = rest - mid
            for p, piece in enumerate((high, mid, low)):
                stats = jnp.where(column == p * heads + h, piece, stats)
        turned = stats.T
        pieces = rows_all // width
        per = 16 // pieces
        block = [turned[0:per, j * width:(j + 1) * width] for j in range(pieces)]
        block = block[0] if pieces == 1 else jnp.concatenate(block, axis=0)
        outs[i][rows_all:rows_all + 16, :] = block.astype(bf16)


def merge_kernel(*refs, sources, rows_all, heads, width):
    parts = refs[:sources]
    out, turn_ref = refs[sources:]
    pieces = rows_all // width
    per = 16 // pieces
    logs = []
    for part in parts:
        block = part[rows_all:rows_all + 16, :].astype(f32)
        block = [block[j * per:(j + 1) * per] for j in range(pieces)]
        block = block[0] if pieces == 1 else jnp.concatenate(block, axis=1)
        logs.append(block[0:heads] + (block[heads:2 * heads] + block[2 * heads:3 * heads]))
    top = functools.reduce(jnp.maximum, logs)
    scales = [jnp.exp(l - top) for l in logs]
    total = functools.reduce(jnp.add, scales)
    turn_ref[...] = jnp.zeros_like(turn_ref)
    for i, scale in enumerate(scales):
        turn_ref[i * heads:(i + 1) * heads, :] = scale / total
    turned = turn_ref[...].T
    for h in range(heads):
        cols = slice(h * HEAD_SIZE, (h + 1) * HEAD_SIZE)
        acc = jnp.zeros((rows_all, HEAD_SIZE), f32)
        for i, part in enumerate(parts):
            at = i * heads + h
            acc = acc + turned[:, at:at + 1] * part[0:rows_all, cols].astype(f32)
        out[:, cols] = acc.astype(bf16)


def project_kernel(mine_ref, other_ref, w_mine_ref, w_other_ref, *out_refs, groups, rows, blocks):
    _, z, r = place()
    y = lax.shift_right_logical(r, 1)
    half = w_other_ref.shape[1]
    cols = half // blocks

    def gather(ref, side):
        found = []
        for group in groups:
            for kk in group:
                at = (lax.bitwise_xor(z, kk) * INNER + side * 2) * rows
                found.append(ref[pl.ds(pl.multiple_of(at, 2 * rows), 2 * rows), :])
        return jnp.concatenate(found, axis=0)

    mine = jnp.concatenate([gather(mine_ref, 1 - y), gather(mine_ref, y)], axis=0)
    other = jnp.concatenate([gather(other_ref, 1 - y), gather(other_ref, y)], axis=0)
    for j in range(blocks):
        here = slice(j * cols, (j + 1) * cols)
        col = pl.multiple_of(lax.bitwise_and(r, 1) * half + j * cols, 128)
        term = jnp.dot(mine, w_mine_ref[:, pl.ds(col, cols)], preferred_element_type=f32)
        term = term + jnp.dot(other, w_other_ref[:, here], preferred_element_type=f32)
        at = 0
        for group, out in zip(groups + groups, out_refs):
            size = 2 * rows * len(group)
            out[:, here] = term[at:at + size].astype(out.dtype)
            at += size


def first_sum_kernel(keep_ref, got_ref, out_ref):
    out_ref[...] = (keep_ref[...] + got_ref[...].astype(f32)).astype(out_ref.dtype)


def last_sum_kernel(keep_ref, got_ref, *refs, rows):
    *parts, mine_ref, other_ref, total_ref = refs
    _, _, r = place()
    c = lax.bitwise_and(r, 1)
    total = keep_ref[...] + got_ref[...].astype(f32)
    for part in parts:
        total = total + part[...].astype(f32)
    total_ref[...] = total
    mine_ref[...] = total_ref[pl.ds(pl.multiple_of(c * rows, rows), rows), :].astype(bf16)
    other_ref[...] = total_ref[pl.ds(pl.multiple_of((1 - c) * rows, rows), rows), :].astype(bf16)


def join_kernel(mine_ref, other_ref, out_ref):
    _, _, r = place()
    c = lax.bitwise_and(r, 1)
    half = mine_ref.shape[1]
    out_ref[:, pl.ds(pl.multiple_of(c * half, 128), half)] = mine_ref[...]
    out_ref[:, pl.ds(pl.multiple_of((1 - c) * half, 128), half)] = other_ref[...]


def layer(query_block, cache_keys, stored_values, live_counts, first_position, out_weight):
    devices = lax.axis_size("seq")
    outer = devices // INNER
    rows = query_block.shape[0]
    rows_all = rows * devices
    keys = cache_keys.shape[0]
    heads = QUERY_HEADS // devices
    width = heads * HEAD_SIZE
    copies = devices // KEY_VALUE_HEADS
    model = out_weight.shape[1]
    half = model // 2
    assert heads * copies == QUERY_HEADS // KEY_VALUE_HEADS and keys <= 256
    blocks = CHUNKS if half % (CHUNKS * 128) == 0 else 1
    shape = jax.ShapeDtypeStruct

    def swap(x, k):
        return lax.ppermute(x, "seq", [(i, i ^ k) for i in range(devices)])

    far_first = list(range(outer - 1, -1, -1))
    order = [outer - 1, 1] + far_first[1:-2] + [0]
    phases = [order[:outer // 2], order[outer // 2:3 * outer // 4], order[3 * outer // 4:]]
    groups = [(0, order), (1, order)] + [(k, p) for p in phases for k in range(2, INNER)]
    outs = [shape((SIDES, outer, rows, width), bf16)] + [shape((outer, rows, width), bf16)] * SIDES
    outs += [
        shape((len(p), 2 * keys + 16, HEAD_SIZE), bf16) for k, p in groups
    ]
    inputs = [query_block, cache_keys, stored_values]
    split = pl.pallas_call(
        functools.partial(split_kernel, outer=outer, width=width, groups=groups, copies=copies),
        out_shape=tuple(outs),
        in_specs=[sspec()] + [pl.BlockSpec(memory_space=pltpu.MemorySpace.HBM)] * 3,
        out_specs=tuple(vspec() for _ in outs),
        scratch_shapes=[pltpu.VMEM(x.shape, x.dtype) for x in inputs]
        + [pltpu.SemaphoreType.DMA((3,))],
        name="split",
        compiler_params=pltpu.CompilerParams(vmem_limit_bytes=8 << 20),
    )(live_counts, *inputs)
    q_own, kv_out = split[1:1 + SIDES], split[1 + SIDES:]
    q_pair = swap(split[0], 1)
    kv_pair = swap(kv_out[1], 1)
    kv_far = [
        {k: swap(kv_out[2 + 2 * i + k - 2], k) for k in range(2, INNER)}
        for i in range(len(phases))
    ]
    pair_q = [jnp.stack([q_own[j], q_pair[j]]) for j in range(SIDES)]
    ys = [
        swap(pair_q[j], k * INNER + 2 * j) if k or j else pair_q[0]
        for k in range(outer) for j in range(SIDES)
    ]

    (w_send,) = call(
        split_weight_kernel, [out_weight],
        [shape((out_weight.shape[0], half), bf16)],
    )
    w_other = swap(w_send, 1)

    partial_of = {}
    for near, kk in enumerate(order):
        i = [kk in p for p in phases].index(True)
        far = phases[i].index(kk)
        (out,) = call(
            functools.partial(
                attention_kernel, outer=outer, begin=(near, near) + (far,) * (INNER - 2),
                offsets=[kk], rows_all=rows_all, keys=keys, heads=heads, width=width,
            ),
            [first_position, *ys, kv_out[0], kv_pair, kv_far[i][2], kv_far[i][3]],
            [shape((rows_all + 16, width), bf16)],
            scratch=[pltpu.VMEM((rows_all, INNER * keys), f32), pltpu.VMEM((rows_all, width), f32)],
            scalars=1, flops=4 * rows_all * INNER * keys * width, limit=16,
        )
        partial_of[kk] = swap(out, kk * INNER) if kk else out

    (merged,) = call(
        functools.partial(merge_kernel, sources=outer, rows_all=rows_all, heads=heads, width=width),
        [partial_of[k] for k in range(outer)], [shape((rows_all, width), bf16)],
        scratch=[pltpu.VMEM((128, rows_all), f32)],
    )
    other = swap(merged, 1)

    span = 2 * rows
    term_groups = [[kk] for kk in far_first]
    terms = call(
        functools.partial(project_kernel, groups=term_groups, rows=rows, blocks=blocks),
        [merged, other, out_weight, w_other],
        [shape((span * len(g), half), bf16) for g in term_groups]
        + [shape((span * len(g), half), f32) for g in term_groups],
        flops=4 * rows_all * width * half, limit=20,
    )
    sends, keeps = terms[:outer], terms[outer:]
    gots = [swap(x, 2) for x in sends]
    parts = []
    for i, kk in enumerate(far_first[:-1]):
        (part,) = call(first_sum_kernel, [keeps[i], gots[i]], [shape((span, half), bf16)])
        parts.append(swap(part, kk * INNER))
    mine, theirs = call(
        functools.partial(last_sum_kernel, rows=rows), [keeps[-1], gots[-1]] + parts,
        [shape((rows, half), bf16)] * 2, scratch=[pltpu.VMEM((span, half), f32)],
    )
    (joined,) = call(join_kernel, [mine, swap(theirs, 1)], [shape((rows, model), bf16)])
    return joined


def solution(mesh):
    in_specs = (
        P(("groups", "seq"), None),
        P(("groups", "seq"), None),
        P(("groups", "seq"), None),
        P(("groups", "seq")),
        P("groups"),
        P("seq", None),
    )
    out_specs = P(("groups", "seq"), None)
    return jax.shard_map(layer, mesh=mesh, in_specs=in_specs, out_specs=out_specs, check_vma=False)
```

```python
import functools

import jax
import jax.numpy as jnp
from jax import lax
from jax.experimental import pallas as pl
from jax.experimental.pallas import tpu as pltpu
from jax.sharding import PartitionSpec as P


QUERY_HEADS = 32
KEY_VALUE_HEADS = 16
HEAD_SIZE = 128
INNER = 4
CHUNKS = 3

score_scale = 168.0 ** (-0.5)
masked_value = -1e30
log2e = 1.4426950408889634
ln2 = 0.6931471805599453


bf16 = jnp.bfloat16
f32 = jnp.float32
VM = pltpu.MemorySpace.VMEM
SM = pltpu.MemorySpace.SMEM


def vspec():
    return pl.BlockSpec(memory_space=VM)


def sspec():
    return pl.BlockSpec(memory_space=SM)


def place():
    me = lax.axis_index("seq")
    return me, lax.shift_right_logical(me, 2), lax.bitwise_and(me, 3)


def call(kernel, ins, outs, scratch=(), scalars=0, flops=0, limit=8):
    in_specs = [sspec()] * scalars + [vspec()] * (len(ins) - scalars)
    moved = sum(a.size * a.dtype.itemsize for a in list(ins) + list(outs))
    return pl.pallas_call(
        kernel,
        out_shape=tuple(outs),
        in_specs=in_specs,
        out_specs=tuple(vspec() for _ in outs),
        scratch_shapes=list(scratch),
        cost_estimate=pl.CostEstimate(flops=flops, transcendentals=0, bytes_accessed=moved),
        compiler_params=pltpu.CompilerParams(vmem_limit_bytes=limit << 20),
    )(*ins)


def split_queries_kernel(q_ref, *q_outs, outer, width):
    _, _, r = place()
    for k, out in enumerate(q_outs):
        for zz in range(outer):
            col = pl.multiple_of((zz * INNER + lax.bitwise_xor(r, k)) * width, width)
            out[zz] = q_ref[:, pl.ds(col, width)]


def split_cache_kernel(live_ref, k_ref, v_ref, *kv_outs, groups, copies):
    _, z, r = place()
    keys = k_ref.shape[0]
    live = jnp.full((16, HEAD_SIZE), live_ref[0], jnp.int32).astype(f32).astype(bf16)
    for (k, offsets), out in zip(groups, kv_outs):
        for i, kk in enumerate(offsets):
            head = lax.bitwise_xor(z, kk) * INNER + lax.bitwise_xor(r, k)
            col = pl.multiple_of((head // copies) * HEAD_SIZE, HEAD_SIZE)
            out[i, 0:keys, :] = k_ref[:, pl.ds(col, HEAD_SIZE)]
            out[i, keys:2 * keys, :] = v_ref[:, pl.ds(col, HEAD_SIZE)]
            out[i, 2 * keys:2 * keys + 16, :] = live


def split_weight_kernel(w_ref, out_ref):
    _, _, r = place()
    half = out_ref.shape[1]
    col = pl.multiple_of((1 - lax.bitwise_and(r, 1)) * half, 128)
    out_ref[...] = w_ref[:, pl.ds(col, half)]


def attention_kernel(first_ref, *refs, outer, first, offsets, rows_all, keys, heads, width):
    ys = refs[:outer]
    kvs = refs[outer:outer + INNER]
    begin = [first, first] + [0] * (INNER - 2)
    outs = refs[outer + INNER:outer + INNER + len(offsets)]
    bias_ref, q_ref = refs[outer + INNER + len(offsets):]
    _, z, r = place()
    rows = rows_all // (outer * INNER)
    q_pos = first_ref[0] + lax.broadcasted_iota(jnp.int32, (rows_all, keys), 0)
    lane = lax.broadcasted_iota(jnp.int32, (rows_all, keys), 1)
    lane_f = lane.astype(f32)
    for k in range(INNER):
        start = (z * INNER + lax.bitwise_xor(r, k)) * keys
        live = kvs[k][0, 2 * keys:2 * keys + 1, :].astype(f32)
        live = jnp.concatenate([live] * (keys // HEAD_SIZE), axis=1)
        allowed = (lane_f < live) & (start + lane <= q_pos)
        bias_ref[:, k * keys:(k + 1) * keys] = jnp.where(allowed, 0.0, masked_value)
    column = lax.broadcasted_iota(jnp.int32, (rows_all, 128), 1)
    for i, kk in enumerate(offsets):
        zz = lax.bitwise_xor(z, kk)
        for k2 in range(outer):
            for k in range(INNER):
                src = lax.bitwise_xor(z, k2) * INNER + lax.bitwise_xor(r, k)
                at = pl.multiple_of(src * rows, rows)
                q_ref[pl.ds(at, rows), :] = ys[k2][k, zz].astype(f32)
        stats = jnp.zeros((rows_all, 128), f32)
        for h in range(heads):
            cols = slice(h * HEAD_SIZE, (h + 1) * HEAD_SIZE)
            query = q_ref[:, cols].astype(bf16)
            scores = []
            for k in range(INNER):
                part = lax.dot_general(
                    query, kvs[k][begin[k] + i, 0:keys, :], (((1,), (1,)), ((), ())),
                    preferred_element_type=f32,
                )
                scores.append(part * (score_scale * log2e) + bias_ref[:, k * keys:(k + 1) * keys])
            top = functools.reduce(jnp.maximum, scores)
            best = jnp.maximum(jnp.max(top, axis=1, keepdims=True), -1e29)
            acc = jnp.zeros((rows_all, HEAD_SIZE), f32)
            sums = jnp.zeros((rows_all, keys), f32)
            for k in range(INNER):
                weights = jnp.exp2(scores[k] - best)
                sums = sums + weights
                acc = acc + jnp.dot(
                    weights.astype(bf16), kvs[k][begin[k] + i, keys:2 * keys, :], preferred_element_type=f32
                )
            total = jnp.sum(sums, axis=1, keepdims=True)
            safe = jnp.where(total > 0, total, 1.0)
            outs[i][0:rows_all, cols] = (acc / safe).astype(bf16)
            logsum = jnp.where(total > 0, best * ln2 + jnp.log(safe), masked_value)
            high = logsum.astype(bf16).astype(f32)
            rest = logsum - high
            mid = rest.astype(bf16).astype(f32)
            low = rest - mid
            for p, piece in enumerate((high, mid, low)):
                stats = jnp.where(column == p * heads + h, piece, stats)
        turned = stats.T
        pieces = rows_all // width
        per = 16 // pieces
        block = [turned[0:per, j * width:(j + 1) * width] for j in range(pieces)]
        block = block[0] if pieces == 1 else jnp.concatenate(block, axis=0)
        outs[i][rows_all:rows_all + 16, :] = block.astype(bf16)


def merge_kernel(*refs, sources, rows_all, heads, width):
    parts = refs[:sources]
    out, turn_ref = refs[sources:]
    pieces = rows_all // width
    per = 16 // pieces
    logs = []
    for part in parts:
        block = part[rows_all:rows_all + 16, :].astype(f32)
        block = [block[j * per:(j + 1) * per] for j in range(pieces)]
        block = block[0] if pieces == 1 else jnp.concatenate(block, axis=1)
        logs.append(block[0:heads] + (block[heads:2 * heads] + block[2 * heads:3 * heads]))
    top = functools.reduce(jnp.maximum, logs)
    scales = [jnp.exp(l - top) for l in logs]
    total = functools.reduce(jnp.add, scales)
    turn_ref[...] = jnp.zeros_like(turn_ref)
    for i, scale in enumerate(scales):
        turn_ref[i * heads:(i + 1) * heads, :] = scale / total
    turned = turn_ref[...].T
    for h in range(heads):
        cols = slice(h * HEAD_SIZE, (h + 1) * HEAD_SIZE)
        acc = jnp.zeros((rows_all, HEAD_SIZE), f32)
        for i, part in enumerate(parts):
            at = i * heads + h
            acc = acc + turned[:, at:at + 1] * part[0:rows_all, cols].astype(f32)
        out[:, cols] = acc.astype(bf16)


def project_kernel(mine_ref, other_ref, w_mine_ref, w_other_ref, *out_refs, groups, rows, blocks):
    _, z, r = place()
    y = lax.shift_right_logical(r, 1)
    half = w_other_ref.shape[1]
    cols = half // blocks

    def gather(ref, side):
        found = []
        for group in groups:
            for kk in group:
                at = (lax.bitwise_xor(z, kk) * INNER + side * 2) * rows
                found.append(ref[pl.ds(pl.multiple_of(at, 2 * rows), 2 * rows), :])
        return jnp.concatenate(found, axis=0)

    mine = jnp.concatenate([gather(mine_ref, 1 - y), gather(mine_ref, y)], axis=0)
    other = jnp.concatenate([gather(other_ref, 1 - y), gather(other_ref, y)], axis=0)
    for j in range(blocks):
        here = slice(j * cols, (j + 1) * cols)
        col = pl.multiple_of(lax.bitwise_and(r, 1) * half + j * cols, 128)
        term = jnp.dot(mine, w_mine_ref[:, pl.ds(col, cols)], preferred_element_type=f32)
        term = term + jnp.dot(other, w_other_ref[:, here], preferred_element_type=f32)
        at = 0
        for group, out in zip(groups + groups, out_refs):
            size = 2 * rows * len(group)
            out[:, here] = term[at:at + size].astype(out.dtype)
            at += size


def first_sum_kernel(keep_ref, got_ref, out_ref):
    out_ref[...] = (keep_ref[...] + got_ref[...].astype(f32)).astype(out_ref.dtype)


def last_sum_kernel(keep_ref, got_ref, *refs, rows):
    *parts, mine_ref, other_ref, total_ref = refs
    _, _, r = place()
    c = lax.bitwise_and(r, 1)
    total = keep_ref[...] + got_ref[...].astype(f32)
    for part in parts:
        total = total + part[...].astype(f32)
    total_ref[...] = total
    mine_ref[...] = total_ref[pl.ds(pl.multiple_of(c * rows, rows), rows), :].astype(bf16)
    other_ref[...] = total_ref[pl.ds(pl.multiple_of((1 - c) * rows, rows), rows), :].astype(bf16)


def join_kernel(mine_ref, other_ref, out_ref):
    _, _, r = place()
    c = lax.bitwise_and(r, 1)
    half = mine_ref.shape[1]
    out_ref[:, pl.ds(pl.multiple_of(c * half, 128), half)] = mine_ref[...]
    out_ref[:, pl.ds(pl.multiple_of((1 - c) * half, 128), half)] = other_ref[...]


def layer(query_block, cache_keys, stored_values, live_counts, first_position, out_weight):
    devices = lax.axis_size("seq")
    outer = devices // INNER
    rows = query_block.shape[0]
    rows_all = rows * devices
    keys = cache_keys.shape[0]
    heads = QUERY_HEADS // devices
    width = heads * HEAD_SIZE
    copies = devices // KEY_VALUE_HEADS
    model = out_weight.shape[1]
    half = model // 2
    assert heads * copies == QUERY_HEADS // KEY_VALUE_HEADS and keys <= 256
    blocks = CHUNKS if half % (CHUNKS * 128) == 0 else 1
    shape = jax.ShapeDtypeStruct

    def swap(x, k):
        return lax.ppermute(x, "seq", [(i, i ^ k) for i in range(devices)])

    order = list(range(outer - 1, -1, -1))
    phases = [order[:outer // 2], order[outer // 2:3 * outer // 4], order[3 * outer // 4:]]
    groups = [(0, order), (1, order)] + [(k, p) for p in phases for k in range(2, INNER)]
    q_out = call(
        functools.partial(split_queries_kernel, outer=outer, width=width),
        [query_block], [shape((outer, rows, width), bf16)] * INNER,
    )
    kv_out = call(
        functools.partial(split_cache_kernel, groups=groups, copies=copies),
        [live_counts, cache_keys, stored_values],
        [shape((len(p), 2 * keys + 16, HEAD_SIZE), bf16) for k, p in groups], scalars=1,
    )
    q_got = {k: swap(q_out[k], k) for k in (2, 3, 1)}
    kv_pair = swap(kv_out[1], 1)
    kv_far = [
        {k: swap(kv_out[2 + 2 * i + k - 2], k) for k in range(2, INNER)}
        for i in range(len(phases))
    ]
    inner_q = jnp.stack([q_out[0], q_got[1], q_got[2], q_got[3]])
    ys = [inner_q] + [swap(inner_q, k * INNER) for k in range(1, outer)]

    (w_send,) = call(
        split_weight_kernel, [out_weight],
        [shape((out_weight.shape[0], half), bf16)],
    )
    w_other = swap(w_send, 1)

    partial_of = {}
    at = 0
    for i, offsets in enumerate(phases):
        size = len(offsets)
        outs = call(
            functools.partial(
                attention_kernel, outer=outer, first=at, offsets=offsets, rows_all=rows_all,
                keys=keys, heads=heads, width=width,
            ),
            [first_position, *ys, kv_out[0], kv_pair, kv_far[i][2], kv_far[i][3]],
            [shape((rows_all + 16, width), bf16)] * size,
            scratch=[pltpu.VMEM((rows_all, INNER * keys), f32), pltpu.VMEM((rows_all, width), f32)],
            scalars=1, flops=4 * rows_all * INNER * keys * width * size, limit=20,
        )
        at += size
        for kk, out in zip(offsets, outs):
            partial_of[kk] = swap(out, kk * INNER) if kk else out

    (merged,) = call(
        functools.partial(merge_kernel, sources=outer, rows_all=rows_all, heads=heads, width=width),
        [partial_of[k] for k in range(outer)], [shape((rows_all, width), bf16)],
        scratch=[pltpu.VMEM((128, rows_all), f32)],
    )
    other = swap(merged, 1)

    span = 2 * rows
    term_groups = [[kk] for kk in order]
    terms = call(
        functools.partial(project_kernel, groups=term_groups, rows=rows, blocks=blocks),
        [merged, other, out_weight, w_other],
        [shape((span * len(g), half), bf16) for g in term_groups]
        + [shape((span * len(g), half), f32) for g in term_groups],
        flops=4 * rows_all * width * half, limit=20,
    )
    sends, keeps = terms[:outer], terms[outer:]
    gots = [swap(x, 2) for x in sends]
    parts = []
    for i, kk in enumerate(order[:-1]):
        (part,) = call(first_sum_kernel, [keeps[i], gots[i]], [shape((span, half), bf16)])
        parts.append(swap(part, kk * INNER))
    mine, theirs = call(
        functools.partial(last_sum_kernel, rows=rows), [keeps[-1], gots[-1]] + parts,
        [shape((rows, half), bf16)] * 2, scratch=[pltpu.VMEM((span, half), f32)],
    )
    (joined,) = call(join_kernel, [mine, swap(theirs, 1)], [shape((rows, model), bf16)])
    return joined


def solution(mesh):
    in_specs = (
        P(("groups", "seq"), None),
        P(("groups", "seq"), None),
        P(("groups", "seq"), None),
        P(("groups", "seq")),
        P("groups"),
        P("seq", None),
    )
    out_specs = P(("groups", "seq"), None)
    return jax.shard_map(layer, mesh=mesh, in_specs=in_specs, out_specs=out_specs, check_vma=False)
```

```python
import functools

import jax
import jax.numpy as jnp
from jax import lax
from jax.experimental import pallas as pl
from jax.experimental.pallas import tpu as pltpu
from jax.sharding import PartitionSpec as P


QUERY_HEADS = 32
KEY_VALUE_HEADS = 16
HEAD_SIZE = 128
INNER = 4
CHUNKS = 3

score_scale = 168.0 ** (-0.5)
masked_value = -1e30
log2e = 1.4426950408889634
ln2 = 0.6931471805599453


bf16 = jnp.bfloat16
f32 = jnp.float32
VM = pltpu.MemorySpace.VMEM
SM = pltpu.MemorySpace.SMEM


def vspec():
    return pl.BlockSpec(memory_space=VM)


def sspec():
    return pl.BlockSpec(memory_space=SM)


def place():
    me = lax.axis_index("seq")
    return me, lax.shift_right_logical(me, 2), lax.bitwise_and(me, 3)


def call(kernel, ins, outs, scratch=(), scalars=0, flops=0, limit=8):
    in_specs = [sspec()] * scalars + [vspec()] * (len(ins) - scalars)
    moved = sum(a.size * a.dtype.itemsize for a in list(ins) + list(outs))
    return pl.pallas_call(
        kernel,
        out_shape=tuple(outs),
        in_specs=in_specs,
        out_specs=tuple(vspec() for _ in outs),
        scratch_shapes=list(scratch),
        cost_estimate=pl.CostEstimate(flops=flops, transcendentals=0, bytes_accessed=moved),
        compiler_params=pltpu.CompilerParams(vmem_limit_bytes=limit << 20),
    )(*ins)


def split_queries_kernel(q_ref, *q_outs, outer, width):
    _, _, r = place()
    for k, out in enumerate(q_outs):
        for zz in range(outer):
            col = pl.multiple_of((zz * INNER + lax.bitwise_xor(r, k)) * width, width)
            out[zz] = q_ref[:, pl.ds(col, width)]


def split_cache_kernel(live_ref, k_hbm, v_hbm, *refs, groups, copies):
    _, z, r = place()
    kv_outs = refs[:len(groups)]
    k_ref, v_ref, sems = refs[len(groups):]
    keys = k_ref.shape[0]
    loads = [
        pltpu.make_async_copy(source, target, sems.at[i])
        for i, (source, target) in enumerate(((k_hbm, k_ref), (v_hbm, v_ref)))
    ]
    for load in loads:
        load.start()
    live = jnp.full((16, HEAD_SIZE), live_ref[0], jnp.int32).astype(f32).astype(bf16)
    for load in loads:
        load.wait()
    for (k, offsets), out in zip(groups, kv_outs):
        for i, kk in enumerate(offsets):
            head = lax.bitwise_xor(z, kk) * INNER + lax.bitwise_xor(r, k)
            col = pl.multiple_of((head // copies) * HEAD_SIZE, HEAD_SIZE)
            out[i, 0:keys, :] = k_ref[:, pl.ds(col, HEAD_SIZE)]
            out[i, keys:2 * keys, :] = v_ref[:, pl.ds(col, HEAD_SIZE)]
            out[i, 2 * keys:2 * keys + 16, :] = live


def split_weight_kernel(w_ref, out_ref):
    _, _, r = place()
    half = out_ref.shape[1]
    col = pl.multiple_of((1 - lax.bitwise_and(r, 1)) * half, 128)
    out_ref[...] = w_ref[:, pl.ds(col, half)]


def attention_kernel(first_ref, *refs, outer, begin, offsets, rows_all, keys, heads, width):
    ys = refs[:outer]
    kvs = refs[outer:outer + INNER]
    outs = refs[outer + INNER:outer + INNER + len(offsets)]
    bias_ref, q_ref = refs[outer + INNER + len(offsets):]
    _, z, r = place()
    rows = rows_all // (outer * INNER)
    q_pos = first_ref[0] + lax.broadcasted_iota(jnp.int32, (rows_all, keys), 0)
    lane = lax.broadcasted_iota(jnp.int32, (rows_all, keys), 1)
    lane_f = lane.astype(f32)
    for k in range(INNER):
        start = (z * INNER + lax.bitwise_xor(r, k)) * keys
        live = kvs[k][0, 2 * keys:2 * keys + 1, :].astype(f32)
        live = jnp.concatenate([live] * (keys // HEAD_SIZE), axis=1)
        allowed = (lane_f < live) & (start + lane <= q_pos)
        bias_ref[:, k * keys:(k + 1) * keys] = jnp.where(allowed, 0.0, masked_value)
    column = lax.broadcasted_iota(jnp.int32, (rows_all, 128), 1)
    for i, kk in enumerate(offsets):
        zz = lax.bitwise_xor(z, kk)
        for k2 in range(outer):
            for k in range(INNER):
                src = lax.bitwise_xor(z, k2) * INNER + lax.bitwise_xor(r, k)
                at = pl.multiple_of(src * rows, rows)
                q_ref[pl.ds(at, rows), :] = ys[k2][k, zz].astype(f32)
        stats = jnp.zeros((rows_all, 128), f32)
        for h in range(heads):
            cols = slice(h * HEAD_SIZE, (h + 1) * HEAD_SIZE)
            query = q_ref[:, cols].astype(bf16)
            scores = []
            for k in range(INNER):
                part = lax.dot_general(
                    query, kvs[k][begin[k] + i, 0:keys, :], (((1,), (1,)), ((), ())),
                    preferred_element_type=f32,
                )
                scores.append(part * (score_scale * log2e) + bias_ref[:, k * keys:(k + 1) * keys])
            top = functools.reduce(jnp.maximum, scores)
            best = jnp.maximum(jnp.max(top, axis=1, keepdims=True), -1e29)
            acc = jnp.zeros((rows_all, HEAD_SIZE), f32)
            sums = jnp.zeros((rows_all, keys), f32)
            for k in range(INNER):
                weights = jnp.exp2(scores[k] - best)
                sums = sums + weights
                acc = acc + jnp.dot(
                    weights.astype(bf16), kvs[k][begin[k] + i, keys:2 * keys, :], preferred_element_type=f32
                )
            total = jnp.sum(sums, axis=1, keepdims=True)
            safe = jnp.where(total > 0, total, 1.0)
            outs[i][0:rows_all, cols] = (acc / safe).astype(bf16)
            logsum = jnp.where(total > 0, best * ln2 + jnp.log(safe), masked_value)
            high = logsum.astype(bf16).astype(f32)
            rest = logsum - high
            mid = rest.astype(bf16).astype(f32)
            low = rest - mid
            for p, piece in enumerate((high, mid, low)):
                stats = jnp.where(column == p * heads + h, piece, stats)
        turned = stats.T
        pieces = rows_all // width
        per = 16 // pieces
        block = [turned[0:per, j * width:(j + 1) * width] for j in range(pieces)]
        block = block[0] if pieces == 1 else jnp.concatenate(block, axis=0)
        outs[i][rows_all:rows_all + 16, :] = block.astype(bf16)


def merge_kernel(*refs, sources, rows_all, heads, width):
    parts = refs[:sources]
    out, turn_ref = refs[sources:]
    pieces = rows_all // width
    per = 16 // pieces
    logs = []
    for part in parts:
        block = part[rows_all:rows_all + 16, :].astype(f32)
        block = [block[j * per:(j + 1) * per] for j in range(pieces)]
        block = block[0] if pieces == 1 else jnp.concatenate(block, axis=1)
        logs.append(block[0:heads] + (block[heads:2 * heads] + block[2 * heads:3 * heads]))
    top = functools.reduce(jnp.maximum, logs)
    scales = [jnp.exp(l - top) for l in logs]
    total = functools.reduce(jnp.add, scales)
    turn_ref[...] = jnp.zeros_like(turn_ref)
    for i, scale in enumerate(scales):
        turn_ref[i * heads:(i + 1) * heads, :] = scale / total
    turned = turn_ref[...].T
    for h in range(heads):
        cols = slice(h * HEAD_SIZE, (h + 1) * HEAD_SIZE)
        acc = jnp.zeros((rows_all, HEAD_SIZE), f32)
        for i, part in enumerate(parts):
            at = i * heads + h
            acc = acc + turned[:, at:at + 1] * part[0:rows_all, cols].astype(f32)
        out[:, cols] = acc.astype(bf16)


def project_kernel(mine_ref, other_ref, w_mine_ref, w_other_ref, *out_refs, groups, rows, blocks):
    _, z, r = place()
    y = lax.shift_right_logical(r, 1)
    half = w_other_ref.shape[1]
    cols = half // blocks

    def gather(ref, side):
        found = []
        for group in groups:
            for kk in group:
                at = (lax.bitwise_xor(z, kk) * INNER + side * 2) * rows
                found.append(ref[pl.ds(pl.multiple_of(at, 2 * rows), 2 * rows), :])
        return jnp.concatenate(found, axis=0)

    mine = jnp.concatenate([gather(mine_ref, 1 - y), gather(mine_ref, y)], axis=0)
    other = jnp.concatenate([gather(other_ref, 1 - y), gather(other_ref, y)], axis=0)
    for j in range(blocks):
        here = slice(j * cols, (j + 1) * cols)
        col = pl.multiple_of(lax.bitwise_and(r, 1) * half + j * cols, 128)
        term = jnp.dot(mine, w_mine_ref[:, pl.ds(col, cols)], preferred_element_type=f32)
        term = term + jnp.dot(other, w_other_ref[:, here], preferred_element_type=f32)
        at = 0
        for group, out in zip(groups + groups, out_refs):
            size = 2 * rows * len(group)
            out[:, here] = term[at:at + size].astype(out.dtype)
            at += size


def first_sum_kernel(keep_ref, got_ref, out_ref):
    out_ref[...] = (keep_ref[...] + got_ref[...].astype(f32)).astype(out_ref.dtype)


def last_sum_kernel(keep_ref, got_ref, *refs, rows):
    *parts, mine_ref, other_ref, total_ref = refs
    _, _, r = place()
    c = lax.bitwise_and(r, 1)
    total = keep_ref[...] + got_ref[...].astype(f32)
    for part in parts:
        total = total + part[...].astype(f32)
    total_ref[...] = total
    mine_ref[...] = total_ref[pl.ds(pl.multiple_of(c * rows, rows), rows), :].astype(bf16)
    other_ref[...] = total_ref[pl.ds(pl.multiple_of((1 - c) * rows, rows), rows), :].astype(bf16)


def join_kernel(mine_ref, other_ref, out_ref):
    _, _, r = place()
    c = lax.bitwise_and(r, 1)
    half = mine_ref.shape[1]
    out_ref[:, pl.ds(pl.multiple_of(c * half, 128), half)] = mine_ref[...]
    out_ref[:, pl.ds(pl.multiple_of((1 - c) * half, 128), half)] = other_ref[...]


def layer(query_block, cache_keys, stored_values, live_counts, first_position, out_weight):
    devices = lax.axis_size("seq")
    outer = devices // INNER
    rows = query_block.shape[0]
    rows_all = rows * devices
    keys = cache_keys.shape[0]
    heads = QUERY_HEADS // devices
    width = heads * HEAD_SIZE
    copies = devices // KEY_VALUE_HEADS
    model = out_weight.shape[1]
    half = model // 2
    assert heads * copies == QUERY_HEADS // KEY_VALUE_HEADS and keys <= 256
    blocks = CHUNKS if half % (CHUNKS * 128) == 0 else 1
    shape = jax.ShapeDtypeStruct

    def swap(x, k):
        return lax.ppermute(x, "seq", [(i, i ^ k) for i in range(devices)])

    order = list(range(outer - 1, -1, -1))
    phases = [order[:outer // 2], order[outer // 2:3 * outer // 4], order[3 * outer // 4:]]
    groups = [(0, order), (1, order)] + [(k, p) for p in phases for k in range(2, INNER)]
    q_out = call(
        functools.partial(split_queries_kernel, outer=outer, width=width),
        [query_block], [shape((outer, rows, width), bf16)] * INNER,
    )
    caches = [pltpu.with_memory_space_constraint(x, pltpu.MemorySpace.HBM) for x in (cache_keys, stored_values)]
    kv_out = pl.pallas_call(
        functools.partial(split_cache_kernel, groups=groups, copies=copies),
        out_shape=tuple(
            shape((len(p), 2 * keys + 16, HEAD_SIZE), bf16) for k, p in groups
        ),
        in_specs=[sspec()] + [pl.BlockSpec(memory_space=pltpu.MemorySpace.HBM)] * 2,
        out_specs=tuple(vspec() for _ in groups),
        scratch_shapes=[pltpu.VMEM(x.shape, x.dtype) for x in caches]
        + [pltpu.SemaphoreType.DMA((2,))],
        name="split_cache",
        compiler_params=pltpu.CompilerParams(vmem_limit_bytes=8 << 20),
    )(live_counts, *caches)
    q_got = {k: swap(q_out[k], k) for k in (2, 3, 1)}
    kv_pair = swap(kv_out[1], 1)
    kv_far = [
        {k: swap(kv_out[2 + 2 * i + k - 2], k) for k in range(2, INNER)}
        for i in range(len(phases))
    ]
    inner_q = jnp.stack([q_out[0], q_got[1], q_got[2], q_got[3]])
    ys = [inner_q] + [swap(inner_q, k * INNER) for k in range(1, outer)]

    (w_send,) = call(
        split_weight_kernel, [out_weight],
        [shape((out_weight.shape[0], half), bf16)],
    )
    w_other = swap(w_send, 1)

    partial_of = {}
    for near, kk in enumerate(order):
        i = [kk in p for p in phases].index(True)
        far = phases[i].index(kk)
        (out,) = call(
            functools.partial(
                attention_kernel, outer=outer, begin=(near, near) + (far,) * (INNER - 2),
                offsets=[kk], rows_all=rows_all, keys=keys, heads=heads, width=width,
            ),
            [first_position, *ys, kv_out[0], kv_pair, kv_far[i][2], kv_far[i][3]],
            [shape((rows_all + 16, width), bf16)],
            scratch=[pltpu.VMEM((rows_all, INNER * keys), f32), pltpu.VMEM((rows_all, width), f32)],
            scalars=1, flops=4 * rows_all * INNER * keys * width, limit=16,
        )
        partial_of[kk] = swap(out, kk * INNER) if kk else out

    (merged,) = call(
        functools.partial(merge_kernel, sources=outer, rows_all=rows_all, heads=heads, width=width),
        [partial_of[k] for k in range(outer)], [shape((rows_all, width), bf16)],
        scratch=[pltpu.VMEM((128, rows_all), f32)],
    )
    other = swap(merged, 1)

    span = 2 * rows
    term_groups = [[kk] for kk in order]
    terms = call(
        functools.partial(project_kernel, groups=term_groups, rows=rows, blocks=blocks),
        [merged, other, out_weight, w_other],
        [shape((span * len(g), half), bf16) for g in term_groups]
        + [shape((span * len(g), half), f32) for g in term_groups],
        flops=4 * rows_all * width * half, limit=20,
    )
    sends, keeps = terms[:outer], terms[outer:]
    gots = [swap(x, 2) for x in sends]
    parts = []
    for i, kk in enumerate(order[:-1]):
        (part,) = call(first_sum_kernel, [keeps[i], gots[i]], [shape((span, half), bf16)])
        parts.append(swap(part, kk * INNER))
    mine, theirs = call(
        functools.partial(last_sum_kernel, rows=rows), [keeps[-1], gots[-1]] + parts,
        [shape((rows, half), bf16)] * 2, scratch=[pltpu.VMEM((span, half), f32)],
    )
    (joined,) = call(join_kernel, [mine, swap(theirs, 1)], [shape((rows, model), bf16)])
    return joined


def solution(mesh):
    in_specs = (
        P(("groups", "seq"), None),
        P(("groups", "seq"), None),
        P(("groups", "seq"), None),
        P(("groups", "seq")),
        P("groups"),
        P("seq", None),
    )
    out_specs = P(("groups", "seq"), None)
    return jax.shard_map(layer, mesh=mesh, in_specs=in_specs, out_specs=out_specs, check_vma=False)
```

```python
import functools

import jax
import jax.numpy as jnp
from jax import lax
from jax.experimental import pallas as pl
from jax.experimental.pallas import tpu as pltpu
from jax.sharding import PartitionSpec as P


QUERY_HEADS = 32
KEY_VALUE_HEADS = 16
HEAD_SIZE = 128
INNER = 4
CHUNKS = 3

score_scale = 168.0 ** (-0.5)
masked_value = -1e30
log2e = 1.4426950408889634
ln2 = 0.6931471805599453


bf16 = jnp.bfloat16
f32 = jnp.float32
VM = pltpu.MemorySpace.VMEM
SM = pltpu.MemorySpace.SMEM


def vspec():
    return pl.BlockSpec(memory_space=VM)


def sspec():
    return pl.BlockSpec(memory_space=SM)


def place():
    me = lax.axis_index("seq")
    return me, lax.shift_right_logical(me, 2), lax.bitwise_and(me, 3)


def call(kernel, ins, outs, scratch=(), scalars=0, flops=0, limit=8):
    in_specs = [sspec()] * scalars + [vspec()] * (len(ins) - scalars)
    moved = sum(a.size * a.dtype.itemsize for a in list(ins) + list(outs))
    return pl.pallas_call(
        kernel,
        out_shape=tuple(outs),
        in_specs=in_specs,
        out_specs=tuple(vspec() for _ in outs),
        scratch_shapes=list(scratch),
        cost_estimate=pl.CostEstimate(flops=flops, transcendentals=0, bytes_accessed=moved),
        compiler_params=pltpu.CompilerParams(vmem_limit_bytes=limit << 20),
    )(*ins)


def split_queries_kernel(q_ref, *q_outs, outer, width):
    _, _, r = place()
    for k, out in enumerate(q_outs):
        for zz in range(outer):
            col = pl.multiple_of((zz * INNER + lax.bitwise_xor(r, k)) * width, width)
            out[zz] = q_ref[:, pl.ds(col, width)]


def split_cache_kernel(live_ref, k_hbm, v_hbm, *refs, groups, copies):
    _, z, r = place()
    kv_outs = refs[:len(groups)]
    k_ref, v_ref, sems = refs[len(groups):]
    keys = k_ref.shape[0]
    loads = [
        pltpu.make_async_copy(source, target, sems.at[i])
        for i, (source, target) in enumerate(((k_hbm, k_ref), (v_hbm, v_ref)))
    ]
    for load in loads:
        load.start()
    live = jnp.full((16, HEAD_SIZE), live_ref[0], jnp.int32).astype(f32).astype(bf16)
    for load in loads:
        load.wait()
    for (k, offsets), out in zip(groups, kv_outs):
        for i, kk in enumerate(offsets):
            head = lax.bitwise_xor(z, kk) * INNER + lax.bitwise_xor(r, k)
            col = pl.multiple_of((head // copies) * HEAD_SIZE, HEAD_SIZE)
            out[i, 0:keys, :] = k_ref[:, pl.ds(col, HEAD_SIZE)]
            out[i, keys:2 * keys, :] = v_ref[:, pl.ds(col, HEAD_SIZE)]
            out[i, 2 * keys:2 * keys + 16, :] = live


def split_weight_kernel(w_ref, out_ref):
    _, _, r = place()
    half = out_ref.shape[1]
    col = pl.multiple_of((1 - lax.bitwise_and(r, 1)) * half, 128)
    out_ref[...] = w_ref[:, pl.ds(col, half)]


def attention_kernel(first_ref, *refs, outer, begin, offsets, rows_all, keys, heads, width):
    ys = refs[:outer]
    kvs = refs[outer:outer + INNER]
    outs = refs[outer + INNER:outer + INNER + len(offsets)]
    bias_ref, q_ref = refs[outer + INNER + len(offsets):]
    _, z, r = place()
    rows = rows_all // (outer * INNER)
    q_pos = first_ref[0] + lax.broadcasted_iota(jnp.int32, (rows_all, keys), 0)
    lane = lax.broadcasted_iota(jnp.int32, (rows_all, keys), 1)
    lane_f = lane.astype(f32)
    for k in range(INNER):
        start = (z * INNER + lax.bitwise_xor(r, k)) * keys
        live = kvs[k][0, 2 * keys:2 * keys + 1, :].astype(f32)
        live = jnp.concatenate([live] * (keys // HEAD_SIZE), axis=1)
        allowed = (lane_f < live) & (start + lane <= q_pos)
        bias_ref[:, k * keys:(k + 1) * keys] = jnp.where(allowed, 0.0, masked_value)
    column = lax.broadcasted_iota(jnp.int32, (rows_all, 128), 1)
    for i, kk in enumerate(offsets):
        zz = lax.bitwise_xor(z, kk)
        for k2 in range(outer):
            for k in range(INNER):
                src = lax.bitwise_xor(z, k2) * INNER + lax.bitwise_xor(r, k)
                at = pl.multiple_of(src * rows, rows)
                q_ref[pl.ds(at, rows), :] = ys[k2][k, zz].astype(f32)
        stats = jnp.zeros((rows_all, 128), f32)
        for h in range(heads):
            cols = slice(h * HEAD_SIZE, (h + 1) * HEAD_SIZE)
            query = q_ref[:, cols].astype(bf16)
            scores = []
            for k in range(INNER):
                part = lax.dot_general(
                    query, kvs[k][begin[k] + i, 0:keys, :], (((1,), (1,)), ((), ())),
                    preferred_element_type=f32,
                )
                scores.append(part * (score_scale * log2e) + bias_ref[:, k * keys:(k + 1) * keys])
            top = functools.reduce(jnp.maximum, scores)
            best = jnp.maximum(jnp.max(top, axis=1, keepdims=True), -1e29)
            acc = jnp.zeros((rows_all, HEAD_SIZE), f32)
            sums = jnp.zeros((rows_all, keys), f32)
            for k in range(INNER):
                weights = jnp.exp2(scores[k] - best)
                sums = sums + weights
                acc = acc + jnp.dot(
                    weights.astype(bf16), kvs[k][begin[k] + i, keys:2 * keys, :], preferred_element_type=f32
                )
            total = jnp.sum(sums, axis=1, keepdims=True)
            safe = jnp.where(total > 0, total, 1.0)
            outs[i][0:rows_all, cols] = (acc / safe).astype(bf16)
            logsum = jnp.where(total > 0, best * ln2 + jnp.log(safe), masked_value)
            high = logsum.astype(bf16).astype(f32)
            rest = logsum - high
            mid = rest.astype(bf16).astype(f32)
            low = rest - mid
            for p, piece in enumerate((high, mid, low)):
                stats = jnp.where(column == p * heads + h, piece, stats)
        turned = stats.T
        pieces = rows_all // width
        per = 16 // pieces
        block = [turned[0:per, j * width:(j + 1) * width] for j in range(pieces)]
        block = block[0] if pieces == 1 else jnp.concatenate(block, axis=0)
        outs[i][rows_all:rows_all + 16, :] = block.astype(bf16)


def merge_kernel(*refs, sources, rows_all, heads, width):
    parts = refs[:sources]
    out, turn_ref = refs[sources:]
    pieces = rows_all // width
    per = 16 // pieces
    logs = []
    for part in parts:
        block = part[rows_all:rows_all + 16, :].astype(f32)
        block = [block[j * per:(j + 1) * per] for j in range(pieces)]
        block = block[0] if pieces == 1 else jnp.concatenate(block, axis=1)
        logs.append(block[0:heads] + (block[heads:2 * heads] + block[2 * heads:3 * heads]))
    top = functools.reduce(jnp.maximum, logs)
    scales = [jnp.exp(l - top) for l in logs]
    total = functools.reduce(jnp.add, scales)
    turn_ref[...] = jnp.zeros_like(turn_ref)
    for i, scale in enumerate(scales):
        turn_ref[i * heads:(i + 1) * heads, :] = scale / total
    turned = turn_ref[...].T
    for h in range(heads):
        cols = slice(h * HEAD_SIZE, (h + 1) * HEAD_SIZE)
        acc = jnp.zeros((rows_all, HEAD_SIZE), f32)
        for i, part in enumerate(parts):
            at = i * heads + h
            acc = acc + turned[:, at:at + 1] * part[0:rows_all, cols].astype(f32)
        out[:, cols] = acc.astype(bf16)


def project_kernel(mine_ref, other_ref, w_mine_ref, w_other_ref, *out_refs, groups, rows, blocks):
    _, z, r = place()
    y = lax.shift_right_logical(r, 1)
    half = w_other_ref.shape[1]
    cols = half // blocks

    def gather(ref, side):
        found = []
        for group in groups:
            for kk in group:
                at = (lax.bitwise_xor(z, kk) * INNER + side * 2) * rows
                found.append(ref[pl.ds(pl.multiple_of(at, 2 * rows), 2 * rows), :])
        return jnp.concatenate(found, axis=0)

    mine = jnp.concatenate([gather(mine_ref, 1 - y), gather(mine_ref, y)], axis=0)
    other = jnp.concatenate([gather(other_ref, 1 - y), gather(other_ref, y)], axis=0)
    for j in range(blocks):
        here = slice(j * cols, (j + 1) * cols)
        col = pl.multiple_of(lax.bitwise_and(r, 1) * half + j * cols, 128)
        term = jnp.dot(mine, w_mine_ref[:, pl.ds(col, cols)], preferred_element_type=f32)
        term = term + jnp.dot(other, w_other_ref[:, here], preferred_element_type=f32)
        at = 0
        for group, out in zip(groups + groups, out_refs):
            size = 2 * rows * len(group)
            out[:, here] = term[at:at + size].astype(out.dtype)
            at += size


def first_sum_kernel(keep_ref, got_ref, out_ref):
    out_ref[...] = (keep_ref[...] + got_ref[...].astype(f32)).astype(out_ref.dtype)


def last_sum_kernel(keep_ref, got_ref, *refs, rows):
    *parts, mine_ref, other_ref, total_ref = refs
    _, _, r = place()
    c = lax.bitwise_and(r, 1)
    total = keep_ref[...] + got_ref[...].astype(f32)
    for part in parts:
        total = total + part[...].astype(f32)
    total_ref[...] = total
    mine_ref[...] = total_ref[pl.ds(pl.multiple_of(c * rows, rows), rows), :].astype(bf16)
    other_ref[...] = total_ref[pl.ds(pl.multiple_of((1 - c) * rows, rows), rows), :].astype(bf16)


def join_kernel(mine_ref, other_ref, out_ref):
    _, _, r = place()
    c = lax.bitwise_and(r, 1)
    half = mine_ref.shape[1]
    out_ref[:, pl.ds(pl.multiple_of(c * half, 128), half)] = mine_ref[...]
    out_ref[:, pl.ds(pl.multiple_of((1 - c) * half, 128), half)] = other_ref[...]


def layer(query_block, cache_keys, stored_values, live_counts, first_position, out_weight):
    devices = lax.axis_size("seq")
    outer = devices // INNER
    rows = query_block.shape[0]
    rows_all = rows * devices
    keys = cache_keys.shape[0]
    heads = QUERY_HEADS // devices
    width = heads * HEAD_SIZE
    copies = devices // KEY_VALUE_HEADS
    model = out_weight.shape[1]
    half = model // 2
    assert heads * copies == QUERY_HEADS // KEY_VALUE_HEADS and keys <= 256
    blocks = CHUNKS if half % (CHUNKS * 128) == 0 else 1
    shape = jax.ShapeDtypeStruct

    def swap(x, k):
        return lax.ppermute(x, "seq", [(i, i ^ k) for i in range(devices)])

    order = list(range(outer - 1, -1, -1))
    phases = [order[:outer // 2], order[outer // 2:3 * outer // 4], order[3 * outer // 4:]]
    groups = [(0, order), (1, order)] + [(k, p) for p in phases for k in range(2, INNER)]
    q_out = call(
        functools.partial(split_queries_kernel, outer=outer, width=width),
        [query_block], [shape((outer, rows, width), bf16)] * INNER,
    )
    caches = [pltpu.with_memory_space_constraint(x, pltpu.MemorySpace.HBM) for x in (cache_keys, stored_values)]
    kv_out = pl.pallas_call(
        functools.partial(split_cache_kernel, groups=groups, copies=copies),
        out_shape=tuple(
            shape((len(p), 2 * keys + 16, HEAD_SIZE), bf16) for k, p in groups
        ),
        in_specs=[sspec()] + [pl.BlockSpec(memory_space=pltpu.MemorySpace.HBM)] * 2,
        out_specs=tuple(vspec() for _ in groups),
        scratch_shapes=[pltpu.VMEM(x.shape, x.dtype) for x in caches]
        + [pltpu.SemaphoreType.DMA((2,))],
        name="split_cache",
        compiler_params=pltpu.CompilerParams(vmem_limit_bytes=8 << 20),
    )(live_counts, *caches)
    q_got = {k: swap(q_out[k], k) for k in (2, 3, 1)}
    kv_pair = swap(kv_out[1], 1)
    kv_far = [
        {k: swap(kv_out[2 + 2 * i + k - 2], k) for k in range(2, INNER)}
        for i in range(len(phases))
    ]
    inner_q = jnp.stack([q_out[0], q_got[1], q_got[2], q_got[3]])
    ys = [inner_q] + [swap(inner_q, k * INNER) for k in range(1, outer)]

    (w_send,) = call(
        split_weight_kernel, [out_weight],
        [shape((out_weight.shape[0], half), bf16)],
    )
    w_other = swap(w_send, 1)

    partial_of = {}
    for near, kk in enumerate(order):
        i = [kk in p for p in phases].index(True)
        far = phases[i].index(kk)
        (out,) = call(
            functools.partial(
                attention_kernel, outer=outer, begin=(near, near) + (far,) * (INNER - 2),
                offsets=[kk], rows_all=rows_all, keys=keys, heads=heads, width=width,
            ),
            [first_position, *ys, kv_out[0], kv_pair, kv_far[i][2], kv_far[i][3]],
            [shape((rows_all + 16, width), bf16)],
            scratch=[pltpu.VMEM((rows_all, INNER * keys), f32), pltpu.VMEM((rows_all, width), f32)],
            scalars=1, flops=4 * rows_all * INNER * keys * width, limit=16,
        )
        partial_of[kk] = swap(out, kk * INNER) if kk else out

    (merged,) = call(
        functools.partial(merge_kernel, sources=outer, rows_all=rows_all, heads=heads, width=width),
        [partial_of[k] for k in range(outer)], [shape((rows_all, width), bf16)],
        scratch=[pltpu.VMEM((128, rows_all), f32)],
    )
    other = swap(merged, 1)

    span = 2 * rows
    turns = [outer - 1, 1] + order[1:-2] + [0]
    term_groups = [[kk] for kk in turns]
    terms = call(
        functools.partial(project_kernel, groups=term_groups, rows=rows, blocks=blocks),
        [merged, other, out_weight, w_other],
        [shape((span * len(g), half), bf16) for g in term_groups]
        + [shape((span * len(g), half), f32) for g in term_groups],
        flops=4 * rows_all * width * half, limit=20,
    )
    sends, keeps = terms[:outer], terms[outer:]
    gots = [swap(x, 2) for x in sends]
    parts = []
    for i, kk in enumerate(turns[:-1]):
        (part,) = call(first_sum_kernel, [keeps[i], gots[i]], [shape((span, half), bf16)])
        parts.append(swap(part, kk * INNER))
    mine, theirs = call(
        functools.partial(last_sum_kernel, rows=rows), [keeps[-1], gots[-1]] + parts,
        [shape((rows, half), bf16)] * 2, scratch=[pltpu.VMEM((span, half), f32)],
    )
    (joined,) = call(join_kernel, [mine, swap(theirs, 1)], [shape((rows, model), bf16)])
    return joined


def solution(mesh):
    in_specs = (
        P(("groups", "seq"), None),
        P(("groups", "seq"), None),
        P(("groups", "seq"), None),
        P(("groups", "seq")),
        P("groups"),
        P("seq", None),
    )
    out_specs = P(("groups", "seq"), None)
    return jax.shard_map(layer, mesh=mesh, in_specs=in_specs, out_specs=out_specs, check_vma=False)
```

```python
import functools

import jax
import jax.numpy as jnp
from jax import lax
from jax.experimental import pallas as pl
from jax.experimental.pallas import tpu as pltpu
from jax.sharding import PartitionSpec as P


QUERY_HEADS = 32
KEY_VALUE_HEADS = 16
HEAD_SIZE = 128
INNER = 4
CHUNKS = 3

score_scale = 168.0 ** (-0.5)
masked_value = -1e30
log2e = 1.4426950408889634
ln2 = 0.6931471805599453


bf16 = jnp.bfloat16
f32 = jnp.float32
VM = pltpu.MemorySpace.VMEM
SM = pltpu.MemorySpace.SMEM


def vspec():
    return pl.BlockSpec(memory_space=VM)


def sspec():
    return pl.BlockSpec(memory_space=SM)


def place():
    me = lax.axis_index("seq")
    return me, lax.shift_right_logical(me, 2), lax.bitwise_and(me, 3)


def call(kernel, ins, outs, scratch=(), scalars=0, flops=0, limit=8):
    in_specs = [sspec()] * scalars + [vspec()] * (len(ins) - scalars)
    moved = sum(a.size * a.dtype.itemsize for a in list(ins) + list(outs))
    return pl.pallas_call(
        kernel,
        out_shape=tuple(outs),
        in_specs=in_specs,
        out_specs=tuple(vspec() for _ in outs),
        scratch_shapes=list(scratch),
        cost_estimate=pl.CostEstimate(flops=flops, transcendentals=0, bytes_accessed=moved),
        compiler_params=pltpu.CompilerParams(vmem_limit_bytes=limit << 20),
    )(*ins)


def split_kernel(live_ref, q_hbm, k_hbm, v_hbm, *refs, outer, width, groups, copies):
    _, z, r = place()
    q_outs = refs[:INNER]
    kv_outs = refs[INNER:INNER + len(groups)]
    q_ref, k_ref, v_ref, sems = refs[INNER + len(groups):]
    keys = k_ref.shape[0]
    loads = [
        pltpu.make_async_copy(source, target, sems.at[i])
        for i, (source, target) in enumerate(((q_hbm, q_ref), (k_hbm, k_ref), (v_hbm, v_ref)))
    ]
    for load in loads:
        load.start()
    live = jnp.full((16, HEAD_SIZE), live_ref[0], jnp.int32).astype(f32).astype(bf16)
    loads[0].wait()
    for k, out in enumerate(q_outs):
        for zz in range(outer):
            col = pl.multiple_of((zz * INNER + lax.bitwise_xor(r, k)) * width, width)
            out[zz] = q_ref[:, pl.ds(col, width)]
    loads[1].wait()
    loads[2].wait()
    for (k, offsets), out in zip(groups, kv_outs):
        for i, kk in enumerate(offsets):
            head = lax.bitwise_xor(z, kk) * INNER + lax.bitwise_xor(r, k)
            col = pl.multiple_of((head // copies) * HEAD_SIZE, HEAD_SIZE)
            out[i, 0:keys, :] = k_ref[:, pl.ds(col, HEAD_SIZE)]
            out[i, keys:2 * keys, :] = v_ref[:, pl.ds(col, HEAD_SIZE)]
            out[i, 2 * keys:2 * keys + 16, :] = live


def split_weight_kernel(w_ref, out_ref):
    _, _, r = place()
    half = out_ref.shape[1]
    col = pl.multiple_of((1 - lax.bitwise_and(r, 1)) * half, 128)
    out_ref[...] = w_ref[:, pl.ds(col, half)]


def attention_kernel(first_ref, *refs, outer, begin, offsets, rows_all, keys, heads, width):
    ys = refs[:outer]
    kvs = refs[outer:outer + INNER]
    outs = refs[outer + INNER:outer + INNER + len(offsets)]
    bias_ref, q_ref = refs[outer + INNER + len(offsets):]
    _, z, r = place()
    rows = rows_all // (outer * INNER)
    q_pos = first_ref[0] + lax.broadcasted_iota(jnp.int32, (rows_all, keys), 0)
    lane = lax.broadcasted_iota(jnp.int32, (rows_all, keys), 1)
    lane_f = lane.astype(f32)
    for k in range(INNER):
        start = (z * INNER + lax.bitwise_xor(r, k)) * keys
        live = kvs[k][0, 2 * keys:2 * keys + 1, :].astype(f32)
        live = jnp.concatenate([live] * (keys // HEAD_SIZE), axis=1)
        allowed = (lane_f < live) & (start + lane <= q_pos)
        bias_ref[:, k * keys:(k + 1) * keys] = jnp.where(allowed, 0.0, masked_value)
    column = lax.broadcasted_iota(jnp.int32, (rows_all, 128), 1)
    for i, kk in enumerate(offsets):
        zz = lax.bitwise_xor(z, kk)
        for k2 in range(outer):
            for k in range(INNER):
                src = lax.bitwise_xor(z, k2) * INNER + lax.bitwise_xor(r, k)
                at = pl.multiple_of(src * rows, rows)
                q_ref[pl.ds(at, rows), :] = ys[k2][k, zz].astype(f32)
        stats = jnp.zeros((rows_all, 128), f32)
        for h in range(heads):
            cols = slice(h * HEAD_SIZE, (h + 1) * HEAD_SIZE)
            query = q_ref[:, cols].astype(bf16)
            scores = []
            for k in range(INNER):
                part = lax.dot_general(
                    query, kvs[k][begin[k] + i, 0:keys, :], (((1,), (1,)), ((), ())),
                    preferred_element_type=f32,
                )
                scores.append(part * (score_scale * log2e) + bias_ref[:, k * keys:(k + 1) * keys])
            top = functools.reduce(jnp.maximum, scores)
            best = jnp.maximum(jnp.max(top, axis=1, keepdims=True), -1e29)
            acc = jnp.zeros((rows_all, HEAD_SIZE), f32)
            sums = jnp.zeros((rows_all, keys), f32)
            for k in range(INNER):
                weights = jnp.exp2(scores[k] - best)
                sums = sums + weights
                acc = acc + jnp.dot(
                    weights.astype(bf16), kvs[k][begin[k] + i, keys:2 * keys, :], preferred_element_type=f32
                )
            total = jnp.sum(sums, axis=1, keepdims=True)
            safe = jnp.where(total > 0, total, 1.0)
            outs[i][0:rows_all, cols] = (acc / safe).astype(bf16)
            logsum = jnp.where(total > 0, best * ln2 + jnp.log(safe), masked_value)
            high = logsum.astype(bf16).astype(f32)
            rest = logsum - high
            mid = rest.astype(bf16).astype(f32)
            low = rest - mid
            for p, piece in enumerate((high, mid, low)):
                stats = jnp.where(column == p * heads + h, piece, stats)
        turned = stats.T
        pieces = rows_all // width
        per = 16 // pieces
        block = [turned[0:per, j * width:(j + 1) * width] for j in range(pieces)]
        block = block[0] if pieces == 1 else jnp.concatenate(block, axis=0)
        outs[i][rows_all:rows_all + 16, :] = block.astype(bf16)


def merge_kernel(*refs, sources, rows_all, heads, width):
    parts = refs[:sources]
    out, turn_ref = refs[sources:]
    pieces = rows_all // width
    per = 16 // pieces
    logs = []
    for part in parts:
        block = part[rows_all:rows_all + 16, :].astype(f32)
        block = [block[j * per:(j + 1) * per] for j in range(pieces)]
        block = block[0] if pieces == 1 else jnp.concatenate(block, axis=1)
        logs.append(block[0:heads] + (block[heads:2 * heads] + block[2 * heads:3 * heads]))
    top = functools.reduce(jnp.maximum, logs)
    scales = [jnp.exp(l - top) for l in logs]
    total = functools.reduce(jnp.add, scales)
    turn_ref[...] = jnp.zeros_like(turn_ref)
    for i, scale in enumerate(scales):
        turn_ref[i * heads:(i + 1) * heads, :] = scale / total
    turned = turn_ref[...].T
    for h in range(heads):
        cols = slice(h * HEAD_SIZE, (h + 1) * HEAD_SIZE)
        acc = jnp.zeros((rows_all, HEAD_SIZE), f32)
        for i, part in enumerate(parts):
            at = i * heads + h
            acc = acc + turned[:, at:at + 1] * part[0:rows_all, cols].astype(f32)
        out[:, cols] = acc.astype(bf16)


def project_kernel(mine_ref, other_ref, w_mine_ref, w_other_ref, *out_refs, groups, rows, blocks):
    _, z, r = place()
    y = lax.shift_right_logical(r, 1)
    half = w_other_ref.shape[1]
    cols = half // blocks

    def gather(ref, side):
        found = []
        for group in groups:
            for kk in group:
                at = (lax.bitwise_xor(z, kk) * INNER + side * 2) * rows
                found.append(ref[pl.ds(pl.multiple_of(at, 2 * rows), 2 * rows), :])
        return jnp.concatenate(found, axis=0)

    mine = jnp.concatenate([gather(mine_ref, 1 - y), gather(mine_ref, y)], axis=0)
    other = jnp.concatenate([gather(other_ref, 1 - y), gather(other_ref, y)], axis=0)
    for j in range(blocks):
        here = slice(j * cols, (j + 1) * cols)
        col = pl.multiple_of(lax.bitwise_and(r, 1) * half + j * cols, 128)
        term = jnp.dot(mine, w_mine_ref[:, pl.ds(col, cols)], preferred_element_type=f32)
        term = term + jnp.dot(other, w_other_ref[:, here], preferred_element_type=f32)
        at = 0
        for group, out in zip(groups + groups, out_refs):
            size = 2 * rows * len(group)
            out[:, here] = term[at:at + size].astype(out.dtype)
            at += size


def first_sum_kernel(keep_ref, got_ref, out_ref):
    out_ref[...] = (keep_ref[...] + got_ref[...].astype(f32)).astype(out_ref.dtype)


def last_sum_kernel(keep_ref, got_ref, *refs, rows):
    *parts, mine_ref, other_ref, total_ref = refs
    _, _, r = place()
    c = lax.bitwise_and(r, 1)
    total = keep_ref[...] + got_ref[...].astype(f32)
    for part in parts:
        total = total + part[...].astype(f32)
    total_ref[...] = total
    mine_ref[...] = total_ref[pl.ds(pl.multiple_of(c * rows, rows), rows), :].astype(bf16)
    other_ref[...] = total_ref[pl.ds(pl.multiple_of((1 - c) * rows, rows), rows), :].astype(bf16)


def join_kernel(mine_ref, other_ref, out_ref):
    _, _, r = place()
    c = lax.bitwise_and(r, 1)
    half = mine_ref.shape[1]
    out_ref[:, pl.ds(pl.multiple_of(c * half, 128), half)] = mine_ref[...]
    out_ref[:, pl.ds(pl.multiple_of((1 - c) * half, 128), half)] = other_ref[...]


def layer(query_block, cache_keys, stored_values, live_counts, first_position, out_weight):
    devices = lax.axis_size("seq")
    outer = devices // INNER
    rows = query_block.shape[0]
    rows_all = rows * devices
    keys = cache_keys.shape[0]
    heads = QUERY_HEADS // devices
    width = heads * HEAD_SIZE
    copies = devices // KEY_VALUE_HEADS
    model = out_weight.shape[1]
    half = model // 2
    assert heads * copies == QUERY_HEADS // KEY_VALUE_HEADS and keys <= 256
    blocks = CHUNKS if half % (CHUNKS * 128) == 0 else 1
    shape = jax.ShapeDtypeStruct

    def swap(x, k):
        return lax.ppermute(x, "seq", [(i, i ^ k) for i in range(devices)])

    order = [outer - 1, 1] + list(range(outer - 2, 1, -1)) + [0]
    phases = [order[:outer // 2], order[outer // 2:3 * outer // 4], order[3 * outer // 4:]]
    groups = [(0, order), (1, order)] + [(k, p) for p in phases for k in range(2, INNER)]
    inputs = [
        pltpu.with_memory_space_constraint(x, pltpu.MemorySpace.HBM)
        for x in (query_block, cache_keys, stored_values)
    ]
    outs = [shape((outer, rows, width), bf16)] * INNER
    outs += [shape((len(p), 2 * keys + 16, HEAD_SIZE), bf16) for k, p in groups]
    split = pl.pallas_call(
        functools.partial(split_kernel, outer=outer, width=width, groups=groups, copies=copies),
        out_shape=tuple(outs),
        in_specs=[sspec()] + [pl.BlockSpec(memory_space=pltpu.MemorySpace.HBM)] * 3,
        out_specs=tuple(vspec() for _ in outs),
        scratch_shapes=[pltpu.VMEM(x.shape, x.dtype) for x in inputs]
        + [pltpu.SemaphoreType.DMA((3,))],
        name="split",
        compiler_params=pltpu.CompilerParams(vmem_limit_bytes=8 << 20),
    )(live_counts, *inputs)
    q_out, kv_out = split[:INNER], split[INNER:]
    q_got = {k: swap(q_out[k], k) for k in (2, 3, 1)}
    kv_pair = swap(kv_out[1], 1)
    kv_far = [
        {k: swap(kv_out[2 + 2 * i + k - 2], k) for k in range(2, INNER)}
        for i in range(len(phases))
    ]
    inner_q = jnp.stack([q_out[0], q_got[1], q_got[2], q_got[3]])
    ys = [inner_q] + [swap(inner_q, k * INNER) for k in range(1, outer)]

    (w_send,) = call(
        split_weight_kernel, [out_weight],
        [shape((out_weight.shape[0], half), bf16)],
    )
    w_other = swap(w_send, 1)

    partial_of = {}
    for near, kk in enumerate(order):
        i = [kk in p for p in phases].index(True)
        far = phases[i].index(kk)
        (out,) = call(
            functools.partial(
                attention_kernel, outer=outer, begin=(near, near) + (far,) * (INNER - 2),
                offsets=[kk], rows_all=rows_all, keys=keys, heads=heads, width=width,
            ),
            [first_position, *ys, kv_out[0], kv_pair, kv_far[i][2], kv_far[i][3]],
            [shape((rows_all + 16, width), bf16)],
            scratch=[pltpu.VMEM((rows_all, INNER * keys), f32), pltpu.VMEM((rows_all, width), f32)],
            scalars=1, flops=4 * rows_all * INNER * keys * width, limit=16,
        )
        partial_of[kk] = swap(out, kk * INNER) if kk else out

    (merged,) = call(
        functools.partial(merge_kernel, sources=outer, rows_all=rows_all, heads=heads, width=width),
        [partial_of[k] for k in range(outer)], [shape((rows_all, width), bf16)],
        scratch=[pltpu.VMEM((128, rows_all), f32)],
    )
    other = swap(merged, 1)

    span = 2 * rows
    term_groups = [[kk] for kk in order]
    terms = call(
        functools.partial(project_kernel, groups=term_groups, rows=rows, blocks=blocks),
        [merged, other, out_weight, w_other],
        [shape((span * len(g), half), bf16) for g in term_groups]
        + [shape((span * len(g), half), f32) for g in term_groups],
        flops=4 * rows_all * width * half, limit=20,
    )
    sends, keeps = terms[:outer], terms[outer:]
    gots = [swap(x, 2) for x in sends]
    parts = []
    for i, kk in enumerate(order[:-1]):
        (part,) = call(first_sum_kernel, [keeps[i], gots[i]], [shape((span, half), bf16)])
        parts.append(swap(part, kk * INNER))
    mine, theirs = call(
        functools.partial(last_sum_kernel, rows=rows), [keeps[-1], gots[-1]] + parts,
        [shape((rows, half), bf16)] * 2, scratch=[pltpu.VMEM((span, half), f32)],
    )
    (joined,) = call(join_kernel, [mine, swap(theirs, 1)], [shape((rows, model), bf16)])
    return joined


def solution(mesh):
    in_specs = (
        P(("groups", "seq"), None),
        P(("groups", "seq"), None),
        P(("groups", "seq"), None),
        P(("groups", "seq")),
        P("groups"),
        P("seq", None),
    )
    out_specs = P(("groups", "seq"), None)
    return jax.shard_map(layer, mesh=mesh, in_specs=in_specs, out_specs=out_specs, check_vma=False)
```

```python
import functools

import jax
import jax.numpy as jnp
from jax import lax
from jax.experimental import pallas as pl
from jax.experimental.pallas import tpu as pltpu
from jax.sharding import PartitionSpec as P


QUERY_HEADS = 32
KEY_VALUE_HEADS = 16
HEAD_SIZE = 128
INNER = 4
EARLY_PART = 20

score_scale = 168.0 ** (-0.5)
masked_value = -1e30
log2e = 1.4426950408889634
ln2 = 0.6931471805599453


bf16 = jnp.bfloat16
f32 = jnp.float32
VM = pltpu.MemorySpace.VMEM
SM = pltpu.MemorySpace.SMEM


def vspec():
    return pl.BlockSpec(memory_space=VM)


def sspec():
    return pl.BlockSpec(memory_space=SM)


def place():
    me = lax.axis_index("seq")
    return me, lax.shift_right_logical(me, 2), lax.bitwise_and(me, 3)


def call(kernel, ins, outs, scratch=(), scalars=0, flops=0, limit=8):
    in_specs = [sspec()] * scalars + [vspec()] * (len(ins) - scalars)
    moved = sum(a.size * a.dtype.itemsize for a in list(ins) + list(outs))
    return pl.pallas_call(
        kernel,
        out_shape=tuple(outs),
        in_specs=in_specs,
        out_specs=tuple(vspec() for _ in outs),
        scratch_shapes=list(scratch),
        cost_estimate=pl.CostEstimate(flops=flops, transcendentals=0, bytes_accessed=moved),
        compiler_params=pltpu.CompilerParams(vmem_limit_bytes=limit << 20),
    )(*ins)


def split_kernel(live_ref, q_hbm, k_hbm, v_hbm, *refs, outer, width, groups, copies):
    _, z, r = place()
    q_outs = refs[:INNER]
    kv_outs = refs[INNER:INNER + len(groups)]
    q_ref, k_ref, v_ref, sems = refs[INNER + len(groups):]
    keys = k_ref.shape[0]
    loads = [
        pltpu.make_async_copy(source, target, sems.at[i])
        for i, (source, target) in enumerate(((q_hbm, q_ref), (k_hbm, k_ref), (v_hbm, v_ref)))
    ]
    for load in loads:
        load.start()
    live = jnp.full((16, HEAD_SIZE), live_ref[0], jnp.int32).astype(f32).astype(bf16)
    loads[0].wait()
    for k, out in enumerate(q_outs):
        for zz in range(outer):
            col = pl.multiple_of((zz * INNER + lax.bitwise_xor(r, k)) * width, width)
            out[zz] = q_ref[:, pl.ds(col, width)]
    loads[1].wait()
    loads[2].wait()
    for (k, offsets), out in zip(groups, kv_outs):
        for i, kk in enumerate(offsets):
            head = lax.bitwise_xor(z, kk) * INNER + lax.bitwise_xor(r, k)
            col = pl.multiple_of((head // copies) * HEAD_SIZE, HEAD_SIZE)
            out[i, 0:keys, :] = k_ref[:, pl.ds(col, HEAD_SIZE)]
            out[i, keys:2 * keys, :] = v_ref[:, pl.ds(col, HEAD_SIZE)]
            out[i, 2 * keys:2 * keys + 16, :] = live


def split_weight_kernel(w_ref, out_ref):
    _, _, r = place()
    half = out_ref.shape[1]
    col = pl.multiple_of((1 - lax.bitwise_and(r, 1)) * half, 128)
    out_ref[...] = w_ref[:, pl.ds(col, half)]


def attention_kernel(first_ref, *refs, outer, begin, offsets, rows_all, keys, heads, width):
    ys = refs[:outer]
    kvs = refs[outer:outer + INNER]
    outs = refs[outer + INNER:outer + INNER + len(offsets)]
    bias_ref, q_ref = refs[outer + INNER + len(offsets):]
    _, z, r = place()
    rows = rows_all // (outer * INNER)
    q_pos = first_ref[0] + lax.broadcasted_iota(jnp.int32, (rows_all, keys), 0)
    lane = lax.broadcasted_iota(jnp.int32, (rows_all, keys), 1)
    lane_f = lane.astype(f32)
    for k in range(INNER):
        start = (z * INNER + lax.bitwise_xor(r, k)) * keys
        live = kvs[k][0, 2 * keys:2 * keys + 1, :].astype(f32)
        live = jnp.concatenate([live] * (keys // HEAD_SIZE), axis=1)
        allowed = (lane_f < live) & (start + lane <= q_pos)
        bias_ref[:, k * keys:(k + 1) * keys] = jnp.where(allowed, 0.0, masked_value)
    column = lax.broadcasted_iota(jnp.int32, (rows_all, 128), 1)
    for i, kk in enumerate(offsets):
        zz = lax.bitwise_xor(z, kk)
        for k2 in range(outer):
            for k in range(INNER):
                src = lax.bitwise_xor(z, k2) * INNER + lax.bitwise_xor(r, k)
                at = pl.multiple_of(src * rows, rows)
                q_ref[pl.ds(at, rows), :] = ys[k2][k, zz].astype(f32)
        stats = jnp.zeros((rows_all, 128), f32)
        for h in range(heads):
            cols = slice(h * HEAD_SIZE, (h + 1) * HEAD_SIZE)
            query = q_ref[:, cols].astype(bf16)
            scores = []
            for k in range(INNER):
                part = lax.dot_general(
                    query, kvs[k][begin[k] + i, 0:keys, :], (((1,), (1,)), ((), ())),
                    preferred_element_type=f32,
                )
                scores.append(part * (score_scale * log2e) + bias_ref[:, k * keys:(k + 1) * keys])
            top = functools.reduce(jnp.maximum, scores)
            best = jnp.maximum(jnp.max(top, axis=1, keepdims=True), -1e29)
            acc = jnp.zeros((rows_all, HEAD_SIZE), f32)
            sums = jnp.zeros((rows_all, keys), f32)
            for k in range(INNER):
                weights = jnp.exp2(scores[k] - best)
                sums = sums + weights
                acc = acc + jnp.dot(
                    weights.astype(bf16), kvs[k][begin[k] + i, keys:2 * keys, :], preferred_element_type=f32
                )
            total = jnp.sum(sums, axis=1, keepdims=True)
            safe = jnp.where(total > 0, total, 1.0)
            outs[i][0:rows_all, cols] = (acc / safe).astype(bf16)
            logsum = jnp.where(total > 0, best * ln2 + jnp.log(safe), masked_value)
            high = logsum.astype(bf16).astype(f32)
            rest = logsum - high
            mid = rest.astype(bf16).astype(f32)
            low = rest - mid
            for p, piece in enumerate((high, mid, low)):
                stats = jnp.where(column == p * heads + h, piece, stats)
        turned = stats.T
        pieces = rows_all // width
        per = 16 // pieces
        block = [turned[0:per, j * width:(j + 1) * width] for j in range(pieces)]
        block = block[0] if pieces == 1 else jnp.concatenate(block, axis=0)
        outs[i][rows_all:rows_all + 16, :] = block.astype(bf16)


def merge_kernel(*refs, sources, rows_all, heads, width):
    parts = refs[:sources]
    out, turn_ref = refs[sources:]
    pieces = rows_all // width
    per = 16 // pieces
    logs = []
    for part in parts:
        block = part[rows_all:rows_all + 16, :].astype(f32)
        block = [block[j * per:(j + 1) * per] for j in range(pieces)]
        block = block[0] if pieces == 1 else jnp.concatenate(block, axis=1)
        logs.append(block[0:heads] + (block[heads:2 * heads] + block[2 * heads:3 * heads]))
    top = functools.reduce(jnp.maximum, logs)
    scales = [jnp.exp(l - top) for l in logs]
    total = functools.reduce(jnp.add, scales)
    turn_ref[...] = jnp.zeros_like(turn_ref)
    for i, scale in enumerate(scales):
        turn_ref[i * heads:(i + 1) * heads, :] = scale / total
    turned = turn_ref[...].T
    for h in range(heads):
        cols = slice(h * HEAD_SIZE, (h + 1) * HEAD_SIZE)
        acc = jnp.zeros((rows_all, HEAD_SIZE), f32)
        for i, part in enumerate(parts):
            at = i * heads + h
            acc = acc + turned[:, at:at + 1] * part[0:rows_all, cols].astype(f32)
        out[:, cols] = acc.astype(bf16)


def project_kernel(
    mine_ref, other_ref, w_mine_ref, w_other_ref, *out_refs, order, outer, rows, early, blocks
):
    _, z, r = place()
    y = lax.shift_right_logical(r, 1)
    half = w_other_ref.shape[1]
    sends, keeps, earlies = out_refs[:outer], out_refs[outer:2 * outer], out_refs[2 * outer:]

    def gather(ref, first, size):
        found = []
        for kk in order:
            at = (lax.bitwise_xor(z, kk) * INNER + first) * rows
            found.append(ref[pl.ds(pl.multiple_of(at, size), size), :])
        return found

    def terms(mine, other, begin, cols):
        col = pl.multiple_of(lax.bitwise_and(r, 1) * half + begin, 128)
        term = jnp.dot(mine, w_mine_ref[:, pl.ds(col, cols)], preferred_element_type=f32)
        return term + jnp.dot(
            other, w_other_ref[:, begin:begin + cols], preferred_element_type=f32
        )

    def store(term, outs, here):
        for i, out in enumerate(outs):
            size = out.shape[0]
            out[:, here] = term[i * size:(i + 1) * size].astype(out.dtype)

    span = 2 * rows
    lines = [
        jnp.concatenate(gather(ref, 2 * (1 - y), span) + gather(ref, 2 * y, span), axis=0)
        for ref in (mine_ref, other_ref)
    ]
    cols = (half - early) // blocks
    for j in range(blocks):
        term = terms(*lines, early + j * cols, cols)
        store(term, sends + keeps, slice(j * cols, (j + 1) * cols))
    lines = [
        jnp.concatenate(gather(ref, 0, INNER * rows), axis=0) for ref in (mine_ref, other_ref)
    ]
    store(terms(*lines, 0, early), earlies, slice(0, early))


def first_sum_kernel(keep_ref, got_ref, out_ref):
    out_ref[...] = (keep_ref[...] + got_ref[...].astype(f32)).astype(out_ref.dtype)


def early_sum_kernel(*refs, span):
    *parts, send_ref, keep_ref, total_ref = refs
    _, _, r = place()
    y = lax.shift_right_logical(r, 1)
    total_ref[...] = functools.reduce(jnp.add, [part[...].astype(f32) for part in parts])
    send_ref[...] = total_ref[pl.ds(pl.multiple_of((1 - y) * span, span), span), :].astype(bf16)
    keep_ref[...] = total_ref[pl.ds(pl.multiple_of(y * span, span), span), :]


def last_sum_kernel(early_keep_ref, early_got_ref, keep_ref, got_ref, *refs, rows):
    *parts, mine_ref, other_ref, total_ref = refs
    _, _, r = place()
    c = lax.bitwise_and(r, 1)
    early = early_keep_ref.shape[1]
    total_ref[:, :early] = early_keep_ref[...] + early_got_ref[...].astype(f32)
    total = keep_ref[...] + got_ref[...].astype(f32)
    for part in parts:
        total = total + part[...].astype(f32)
    total_ref[:, early:] = total
    mine_ref[...] = total_ref[pl.ds(pl.multiple_of(c * rows, rows), rows), :].astype(bf16)
    other_ref[...] = total_ref[pl.ds(pl.multiple_of((1 - c) * rows, rows), rows), :].astype(bf16)


def join_kernel(mine_ref, other_ref, out_ref):
    _, _, r = place()
    c = lax.bitwise_and(r, 1)
    half = mine_ref.shape[1]
    out_ref[:, pl.ds(pl.multiple_of(c * half, 128), half)] = mine_ref[...]
    out_ref[:, pl.ds(pl.multiple_of((1 - c) * half, 128), half)] = other_ref[...]


def layer(query_block, cache_keys, stored_values, live_counts, first_position, out_weight):
    devices = lax.axis_size("seq")
    outer = devices // INNER
    rows = query_block.shape[0]
    rows_all = rows * devices
    keys = cache_keys.shape[0]
    heads = QUERY_HEADS // devices
    width = heads * HEAD_SIZE
    copies = devices // KEY_VALUE_HEADS
    model = out_weight.shape[1]
    half = model // 2
    assert heads * copies == QUERY_HEADS // KEY_VALUE_HEADS and keys <= 256
    tiles = half // 128
    early = 128 * (tiles * EARLY_PART // 100)
    blocks = 2 if (half - early) % 256 == 0 else 1
    shape = jax.ShapeDtypeStruct

    def swap(x, k):
        return lax.ppermute(x, "seq", [(i, i ^ k) for i in range(devices)])

    order = [outer - 1, 1] + list(range(outer - 2, 1, -1)) + [0]
    phases = [order[:outer // 2], order[outer // 2:3 * outer // 4], order[3 * outer // 4:]]
    groups = [(0, order), (1, order)] + [(k, p) for p in phases for k in range(2, INNER)]
    inputs = [
        pltpu.with_memory_space_constraint(x, pltpu.MemorySpace.HBM)
        for x in (query_block, cache_keys, stored_values)
    ]
    outs = [shape((outer, rows, width), bf16)] * INNER
    outs += [shape((len(p), 2 * keys + 16, HEAD_SIZE), bf16) for k, p in groups]
    split = pl.pallas_call(
        functools.partial(split_kernel, outer=outer, width=width, groups=groups, copies=copies),
        out_shape=tuple(outs),
        in_specs=[sspec()] + [pl.BlockSpec(memory_space=pltpu.MemorySpace.HBM)] * 3,
        out_specs=tuple(vspec() for _ in outs),
        scratch_shapes=[pltpu.VMEM(x.shape, x.dtype) for x in inputs]
        + [pltpu.SemaphoreType.DMA((3,))],
        name="split",
        compiler_params=pltpu.CompilerParams(vmem_limit_bytes=8 << 20),
    )(live_counts, *inputs)
    q_out, kv_out = split[:INNER], split[INNER:]
    q_got = {k: swap(q_out[k], k) for k in (2, 3, 1)}
    kv_pair = swap(kv_out[1], 1)
    kv_far = [
        {k: swap(kv_out[2 + 2 * i + k - 2], k) for k in range(2, INNER)}
        for i in range(len(phases))
    ]
    inner_q = jnp.stack([q_out[0], q_got[1], q_got[2], q_got[3]])
    ys = [inner_q] + [swap(inner_q, k * INNER) for k in range(1, outer)]

    (w_send,) = call(
        split_weight_kernel, [out_weight],
        [shape((out_weight.shape[0], half), bf16)],
    )
    w_other = swap(w_send, 1)

    partial_of = {}
    for near, kk in enumerate(order):
        i = [kk in p for p in phases].index(True)
        far = phases[i].index(kk)
        (out,) = call(
            functools.partial(
                attention_kernel, outer=outer, begin=(near, near) + (far,) * (INNER - 2),
                offsets=[kk], rows_all=rows_all, keys=keys, heads=heads, width=width,
            ),
            [first_position, *ys, kv_out[0], kv_pair, kv_far[i][2], kv_far[i][3]],
            [shape((rows_all + 16, width), bf16)],
            scratch=[pltpu.VMEM((rows_all, INNER * keys), f32), pltpu.VMEM((rows_all, width), f32)],
            scalars=1, flops=4 * rows_all * INNER * keys * width, limit=16,
        )
        partial_of[kk] = swap(out, kk * INNER) if kk else out

    (merged,) = call(
        functools.partial(merge_kernel, sources=outer, rows_all=rows_all, heads=heads, width=width),
        [partial_of[k] for k in range(outer)], [shape((rows_all, width), bf16)],
        scratch=[pltpu.VMEM((128, rows_all), f32)],
    )
    other = swap(merged, 1)

    span = 2 * rows
    main = half - early
    terms = call(
        functools.partial(
            project_kernel, order=order, outer=outer, rows=rows, early=early, blocks=blocks
        ),
        [merged, other, out_weight, w_other],
        [shape((span, main), bf16)] * outer + [shape((span, main), f32)] * outer
        + [shape((2 * span, early), bf16)] * (outer - 1) + [shape((2 * span, early), f32)],
        flops=4 * rows_all * width * half, limit=20,
    )
    sends, keeps, earlies = terms[:outer], terms[outer:2 * outer], terms[2 * outer:]
    gots = [swap(x, 2) for x in sends]
    early_gots = [swap(x, kk * INNER) for kk, x in zip(order[:-1], earlies)]
    parts = []
    for i, kk in enumerate(order[:-1]):
        (part,) = call(first_sum_kernel, [keeps[i], gots[i]], [shape((span, main), bf16)])
        parts.append(swap(part, kk * INNER))
    early_send, early_keep = call(
        functools.partial(early_sum_kernel, span=span),
        [earlies[-1]] + early_gots, [shape((span, early), bf16), shape((span, early), f32)],
        scratch=[pltpu.VMEM((2 * span, early), f32)],
    )
    mine, theirs = call(
        functools.partial(last_sum_kernel, rows=rows),
        [early_keep, swap(early_send, 2), keeps[-1], gots[-1]] + parts,
        [shape((rows, half), bf16)] * 2, scratch=[pltpu.VMEM((span, half), f32)],
    )
    (joined,) = call(join_kernel, [mine, swap(theirs, 1)], [shape((rows, model), bf16)])
    return joined


def solution(mesh):
    in_specs = (
        P(("groups", "seq"), None),
        P(("groups", "seq"), None),
        P(("groups", "seq"), None),
        P(("groups", "seq")),
        P("groups"),
        P("seq", None),
    )
    out_specs = P(("groups", "seq"), None)
    return jax.shard_map(layer, mesh=mesh, in_specs=in_specs, out_specs=out_specs, check_vma=False)
```

```python
import functools

import jax
import jax.numpy as jnp
from jax import lax
from jax.experimental import pallas as pl
from jax.experimental.pallas import tpu as pltpu
from jax.sharding import PartitionSpec as P


QUERY_HEADS = 32
KEY_VALUE_HEADS = 16
HEAD_SIZE = 128
INNER = 4
EARLY_PART = 24

score_scale = 168.0 ** (-0.5)
masked_value = -1e30
log2e = 1.4426950408889634
ln2 = 0.6931471805599453


bf16 = jnp.bfloat16
f32 = jnp.float32
VM = pltpu.MemorySpace.VMEM
SM = pltpu.MemorySpace.SMEM


def vspec():
    return pl.BlockSpec(memory_space=VM)


def sspec():
    return pl.BlockSpec(memory_space=SM)


def place():
    me = lax.axis_index("seq")
    return me, lax.shift_right_logical(me, 2), lax.bitwise_and(me, 3)


def call(kernel, ins, outs, scratch=(), scalars=0, flops=0, limit=8):
    in_specs = [sspec()] * scalars + [vspec()] * (len(ins) - scalars)
    moved = sum(a.size * a.dtype.itemsize for a in list(ins) + list(outs))
    return pl.pallas_call(
        kernel,
        out_shape=tuple(outs),
        in_specs=in_specs,
        out_specs=tuple(vspec() for _ in outs),
        scratch_shapes=list(scratch),
        cost_estimate=pl.CostEstimate(flops=flops, transcendentals=0, bytes_accessed=moved),
        compiler_params=pltpu.CompilerParams(vmem_limit_bytes=limit << 20),
    )(*ins)


def split_kernel(live_ref, q_hbm, k_hbm, v_hbm, *refs, outer, width, groups, copies):
    _, z, r = place()
    q_outs = refs[:INNER]
    kv_outs = refs[INNER:INNER + len(groups)]
    q_ref, k_ref, v_ref, sems = refs[INNER + len(groups):]
    keys = k_ref.shape[0]
    loads = [
        pltpu.make_async_copy(source, target, sems.at[i])
        for i, (source, target) in enumerate(((q_hbm, q_ref), (k_hbm, k_ref), (v_hbm, v_ref)))
    ]
    for load in loads:
        load.start()
    live = jnp.full((16, HEAD_SIZE), live_ref[0], jnp.int32).astype(f32).astype(bf16)
    loads[0].wait()
    for k, out in enumerate(q_outs):
        for zz in range(outer):
            col = pl.multiple_of((zz * INNER + lax.bitwise_xor(r, k)) * width, width)
            out[zz] = q_ref[:, pl.ds(col, width)]
    loads[1].wait()
    loads[2].wait()
    for (k, offsets), out in zip(groups, kv_outs):
        for i, kk in enumerate(offsets):
            head = lax.bitwise_xor(z, kk) * INNER + lax.bitwise_xor(r, k)
            col = pl.multiple_of((head // copies) * HEAD_SIZE, HEAD_SIZE)
            out[i, 0:keys, :] = k_ref[:, pl.ds(col, HEAD_SIZE)]
            out[i, keys:2 * keys, :] = v_ref[:, pl.ds(col, HEAD_SIZE)]
            out[i, 2 * keys:2 * keys + 16, :] = live


def split_weight_kernel(w_ref, out_ref):
    _, _, r = place()
    half = out_ref.shape[1]
    col = pl.multiple_of((1 - lax.bitwise_and(r, 1)) * half, 128)
    out_ref[...] = w_ref[:, pl.ds(col, half)]


def attention_kernel(first_ref, *refs, outer, begin, offsets, rows_all, keys, heads, width):
    ys = refs[:outer]
    kvs = refs[outer:outer + INNER]
    outs = refs[outer + INNER:outer + INNER + len(offsets)]
    bias_ref, q_ref = refs[outer + INNER + len(offsets):]
    _, z, r = place()
    rows = rows_all // (outer * INNER)
    q_pos = first_ref[0] + lax.broadcasted_iota(jnp.int32, (rows_all, keys), 0)
    lane = lax.broadcasted_iota(jnp.int32, (rows_all, keys), 1)
    lane_f = lane.astype(f32)
    for k in range(INNER):
        start = (z * INNER + lax.bitwise_xor(r, k)) * keys
        live = kvs[k][0, 2 * keys:2 * keys + 1, :].astype(f32)
        live = jnp.concatenate([live] * (keys // HEAD_SIZE), axis=1)
        allowed = (lane_f < live) & (start + lane <= q_pos)
        bias_ref[:, k * keys:(k + 1) * keys] = jnp.where(allowed, 0.0, masked_value)
    column = lax.broadcasted_iota(jnp.int32, (rows_all, 128), 1)
    for i, kk in enumerate(offsets):
        zz = lax.bitwise_xor(z, kk)
        for k2 in range(outer):
            for k in range(INNER):
                src = lax.bitwise_xor(z, k2) * INNER + lax.bitwise_xor(r, k)
                at = pl.multiple_of(src * rows, rows)
                q_ref[pl.ds(at, rows), :] = ys[k2][k, zz].astype(f32)
        stats = jnp.zeros((rows_all, 128), f32)
        for h in range(heads):
            cols = slice(h * HEAD_SIZE, (h + 1) * HEAD_SIZE)
            query = q_ref[:, cols].astype(bf16)
            scores = []
            for k in range(INNER):
                part = lax.dot_general(
                    query, kvs[k][begin[k] + i, 0:keys, :], (((1,), (1,)), ((), ())),
                    preferred_element_type=f32,
                )
                scores.append(part * (score_scale * log2e) + bias_ref[:, k * keys:(k + 1) * keys])
            top = functools.reduce(jnp.maximum, scores)
            best = jnp.maximum(jnp.max(top, axis=1, keepdims=True), -1e29)
            acc = jnp.zeros((rows_all, HEAD_SIZE), f32)
            sums = jnp.zeros((rows_all, keys), f32)
            for k in range(INNER):
                weights = jnp.exp2(scores[k] - best)
                sums = sums + weights
                acc = acc + jnp.dot(
                    weights.astype(bf16), kvs[k][begin[k] + i, keys:2 * keys, :], preferred_element_type=f32
                )
            total = jnp.sum(sums, axis=1, keepdims=True)
            safe = jnp.where(total > 0, total, 1.0)
            outs[i][0:rows_all, cols] = (acc / safe).astype(bf16)
            logsum = jnp.where(total > 0, best * ln2 + jnp.log(safe), masked_value)
            high = logsum.astype(bf16).astype(f32)
            rest = logsum - high
            mid = rest.astype(bf16).astype(f32)
            low = rest - mid
            for p, piece in enumerate((high, mid, low)):
                stats = jnp.where(column == p * heads + h, piece, stats)
        turned = stats.T
        pieces = rows_all // width
        per = 16 // pieces
        block = [turned[0:per, j * width:(j + 1) * width] for j in range(pieces)]
        block = block[0] if pieces == 1 else jnp.concatenate(block, axis=0)
        outs[i][rows_all:rows_all + 16, :] = block.astype(bf16)


def merge_kernel(*refs, sources, rows_all, heads, width):
    parts = refs[:sources]
    out, turn_ref = refs[sources:]
    pieces = rows_all // width
    per = 16 // pieces
    logs = []
    for part in parts:
        block = part[rows_all:rows_all + 16, :].astype(f32)
        block = [block[j * per:(j + 1) * per] for j in range(pieces)]
        block = block[0] if pieces == 1 else jnp.concatenate(block, axis=1)
        logs.append(block[0:heads] + (block[heads:2 * heads] + block[2 * heads:3 * heads]))
    top = functools.reduce(jnp.maximum, logs)
    scales = [jnp.exp(l - top) for l in logs]
    total = functools.reduce(jnp.add, scales)
    turn_ref[...] = jnp.zeros_like(turn_ref)
    for i, scale in enumerate(scales):
        turn_ref[i * heads:(i + 1) * heads, :] = scale / total
    turned = turn_ref[...].T
    for h in range(heads):
        cols = slice(h * HEAD_SIZE, (h + 1) * HEAD_SIZE)
        acc = jnp.zeros((rows_all, HEAD_SIZE), f32)
        for i, part in enumerate(parts):
            at = i * heads + h
            acc = acc + turned[:, at:at + 1] * part[0:rows_all, cols].astype(f32)
        out[:, cols] = acc.astype(bf16)


def project_kernel(
    mine_ref, other_ref, w_mine_ref, w_other_ref, *out_refs, order, outer, rows, early, blocks
):
    _, z, r = place()
    y = lax.shift_right_logical(r, 1)
    half = w_other_ref.shape[1]
    sends, keeps, earlies = out_refs[:outer], out_refs[outer:2 * outer], out_refs[2 * outer:]
    span = 2 * rows
    far = [kk for kk in order if kk >= outer // 2]

    def gather(picks):
        found = []
        for ref in (mine_ref, other_ref):
            lines = []
            for kk, first, size in picks:
                at = (lax.bitwise_xor(z, kk) * INNER + first) * rows
                lines.append(ref[pl.ds(pl.multiple_of(at, size), size), :])
            found.append(jnp.concatenate(lines, axis=0))
        return found

    def terms(lines, begin, cols):
        col = pl.multiple_of(lax.bitwise_and(r, 1) * half + begin, 128)
        term = jnp.dot(lines[0], w_mine_ref[:, pl.ds(col, cols)], preferred_element_type=f32)
        return term + jnp.dot(
            lines[1], w_other_ref[:, begin:begin + cols], preferred_element_type=f32
        )

    sides = [(2 * (1 - y), sends), (2 * y, keeps)]
    lines = gather([(kk, first, span) for first, outs in sides for kk in order])
    cols = (half - early) // blocks
    for j in range(blocks):
        term = terms(lines, early + j * cols, cols)
        for i, out in enumerate(sends + keeps):
            at = j * cols + out.shape[1] - (half - early)
            out[:, at:at + cols] = term[i * span:(i + 1) * span].astype(out.dtype)
    near = [(kk, first, outs[i]) for first, outs in sides for i, kk in enumerate(order)
            if kk not in far]
    picks = [(kk, 0, 2 * span) for kk in far] + [(kk, first, span) for kk, first, out in near]
    term = terms(gather(picks), 0, early)
    at = 0
    for out in list(earlies) + [out for kk, first, out in near]:
        out[:, 0:early] = term[at:at + out.shape[0]].astype(out.dtype)
        at += out.shape[0]


def first_sum_kernel(keep_ref, got_ref, out_ref):
    out_ref[...] = (keep_ref[...] + got_ref[...].astype(f32)).astype(out_ref.dtype)


def early_sum_kernel(*refs, span):
    *parts, send_ref, keep_ref, total_ref = refs
    _, _, r = place()
    y = lax.shift_right_logical(r, 1)
    total_ref[...] = functools.reduce(jnp.add, [part[...].astype(f32) for part in parts])
    send_ref[...] = total_ref[pl.ds(pl.multiple_of((1 - y) * span, span), span), :].astype(bf16)
    keep_ref[...] = total_ref[pl.ds(pl.multiple_of(y * span, span), span), :]


def last_sum_kernel(early_keep_ref, early_got_ref, keep_ref, got_ref, *refs, rows):
    *parts, mine_ref, other_ref, total_ref = refs
    _, _, r = place()
    c = lax.bitwise_and(r, 1)
    early = early_keep_ref.shape[1]
    half = keep_ref.shape[1]
    total = keep_ref[...] + got_ref[...].astype(f32)
    for part in parts:
        if part.shape[1] == half:
            total = total + part[...].astype(f32)
    total_ref[:, :early] = total[:, :early] + early_keep_ref[...] + early_got_ref[...].astype(f32)
    total = total[:, early:]
    for part in parts:
        if part.shape[1] != half:
            total = total + part[...].astype(f32)
    total_ref[:, early:] = total
    mine_ref[...] = total_ref[pl.ds(pl.multiple_of(c * rows, rows), rows), :].astype(bf16)
    other_ref[...] = total_ref[pl.ds(pl.multiple_of((1 - c) * rows, rows), rows), :].astype(bf16)


def join_kernel(mine_ref, other_ref, out_ref):
    _, _, r = place()
    c = lax.bitwise_and(r, 1)
    half = mine_ref.shape[1]
    out_ref[:, pl.ds(pl.multiple_of(c * half, 128), half)] = mine_ref[...]
    out_ref[:, pl.ds(pl.multiple_of((1 - c) * half, 128), half)] = other_ref[...]


def layer(query_block, cache_keys, stored_values, live_counts, first_position, out_weight):
    devices = lax.axis_size("seq")
    outer = devices // INNER
    rows = query_block.shape[0]
    rows_all = rows * devices
    keys = cache_keys.shape[0]
    heads = QUERY_HEADS // devices
    width = heads * HEAD_SIZE
    copies = devices // KEY_VALUE_HEADS
    model = out_weight.shape[1]
    half = model // 2
    assert heads * copies == QUERY_HEADS // KEY_VALUE_HEADS and keys <= 256
    tiles = half // 128
    early = 128 * (tiles * EARLY_PART // 100)
    blocks = next(b for b in (2, 3, 1) if (half - early) % (128 * b) == 0)
    shape = jax.ShapeDtypeStruct

    def swap(x, k):
        return lax.ppermute(x, "seq", [(i, i ^ k) for i in range(devices)])

    order = [outer - 1, 1] + list(range(outer - 2, 1, -1)) + [0]
    phases = [order[:outer // 2], order[outer // 2:3 * outer // 4], order[3 * outer // 4:]]
    groups = [(0, order), (1, order)] + [(k, p) for p in phases for k in range(2, INNER)]
    inputs = [
        pltpu.with_memory_space_constraint(x, pltpu.MemorySpace.HBM)
        for x in (query_block, cache_keys, stored_values)
    ]
    outs = [shape((outer, rows, width), bf16)] * INNER
    outs += [shape((len(p), 2 * keys + 16, HEAD_SIZE), bf16) for k, p in groups]
    split = pl.pallas_call(
        functools.partial(split_kernel, outer=outer, width=width, groups=groups, copies=copies),
        out_shape=tuple(outs),
        in_specs=[sspec()] + [pl.BlockSpec(memory_space=pltpu.MemorySpace.HBM)] * 3,
        out_specs=tuple(vspec() for _ in outs),
        scratch_shapes=[pltpu.VMEM(x.shape, x.dtype) for x in inputs]
        + [pltpu.SemaphoreType.DMA((3,))],
        name="split",
        compiler_params=pltpu.CompilerParams(vmem_limit_bytes=8 << 20),
    )(live_counts, *inputs)
    q_out, kv_out = split[:INNER], split[INNER:]
    q_got = {k: swap(q_out[k], k) for k in (2, 3, 1)}
    kv_pair = swap(kv_out[1], 1)
    kv_far = [
        {k: swap(kv_out[2 + 2 * i + k - 2], k) for k in range(2, INNER)}
        for i in range(len(phases))
    ]
    inner_q = jnp.stack([q_out[0], q_got[1], q_got[2], q_got[3]])
    ys = [inner_q] + [swap(inner_q, k * INNER) for k in range(1, outer)]

    (w_send,) = call(
        split_weight_kernel, [out_weight],
        [shape((out_weight.shape[0], half), bf16)],
    )
    w_other = swap(w_send, 1)

    partial_of = {}
    for near, kk in enumerate(order):
        i = [kk in p for p in phases].index(True)
        far = phases[i].index(kk)
        (out,) = call(
            functools.partial(
                attention_kernel, outer=outer, begin=(near, near) + (far,) * (INNER - 2),
                offsets=[kk], rows_all=rows_all, keys=keys, heads=heads, width=width,
            ),
            [first_position, *ys, kv_out[0], kv_pair, kv_far[i][2], kv_far[i][3]],
            [shape((rows_all + 16, width), bf16)],
            scratch=[pltpu.VMEM((rows_all, INNER * keys), f32), pltpu.VMEM((rows_all, width), f32)],
            scalars=1, flops=4 * rows_all * INNER * keys * width, limit=16,
        )
        partial_of[kk] = swap(out, kk * INNER) if kk else out

    (merged,) = call(
        functools.partial(merge_kernel, sources=outer, rows_all=rows_all, heads=heads, width=width),
        [partial_of[k] for k in range(outer)], [shape((rows_all, width), bf16)],
        scratch=[pltpu.VMEM((128, rows_all), f32)],
    )
    other = swap(merged, 1)

    span = 2 * rows
    far = [kk for kk in order if kk >= outer // 2]
    widths = [half - early if kk in far else half for kk in order]
    terms = call(
        functools.partial(
            project_kernel, order=order, outer=outer, rows=rows, early=early, blocks=blocks
        ),
        [merged, other, out_weight, w_other],
        [shape((span, w), bf16) for w in widths] + [shape((span, w), f32) for w in widths]
        + [shape((2 * span, early), bf16)] * len(far),
        flops=4 * rows_all * width * half, limit=20,
    )
    sends, keeps, earlies = terms[:outer], terms[outer:2 * outer], terms[2 * outer:]
    gots = [swap(x, 2) for x in sends]
    early_gots = [swap(x, kk * INNER) for kk, x in zip(far, earlies)]
    parts = []
    for i, kk in enumerate(order[:-1]):
        (part,) = call(
            first_sum_kernel, [keeps[i], gots[i]],
            [shape((span, widths[i]), bf16)],
        )
        parts.append(swap(part, kk * INNER))
    early_send, early_keep = call(
        functools.partial(early_sum_kernel, span=span),
        early_gots, [shape((span, early), bf16), shape((span, early), f32)],
        scratch=[pltpu.VMEM((2 * span, early), f32)],
    )
    mine, theirs = call(
        functools.partial(last_sum_kernel, rows=rows),
        [early_keep, swap(early_send, 2), keeps[-1], gots[-1]] + parts,
        [shape((rows, half), bf16)] * 2, scratch=[pltpu.VMEM((span, half), f32)],
    )
    (joined,) = call(join_kernel, [mine, swap(theirs, 1)], [shape((rows, model), bf16)])
    return joined


def solution(mesh):
    in_specs = (
        P(("groups", "seq"), None),
        P(("groups", "seq"), None),
        P(("groups", "seq"), None),
        P(("groups", "seq")),
        P("groups"),
        P("seq", None),
    )
    out_specs = P(("groups", "seq"), None)
    return jax.shard_map(layer, mesh=mesh, in_specs=in_specs, out_specs=out_specs, check_vma=False)
```

```python
import functools

import jax
import jax.numpy as jnp
from jax import lax
from jax.experimental import pallas as pl
from jax.experimental.pallas import tpu as pltpu
from jax.sharding import PartitionSpec as P


QUERY_HEADS = 32
KEY_VALUE_HEADS = 16
HEAD_SIZE = 128
INNER = 4
EARLY_PART = 24

score_scale = 168.0 ** (-0.5)
masked_value = -1e30
log2e = 1.4426950408889634
ln2 = 0.6931471805599453


bf16 = jnp.bfloat16
f32 = jnp.float32
VM = pltpu.MemorySpace.VMEM
SM = pltpu.MemorySpace.SMEM


def vspec():
    return pl.BlockSpec(memory_space=VM)


def sspec():
    return pl.BlockSpec(memory_space=SM)


def place():
    me = lax.axis_index("seq")
    return me, lax.shift_right_logical(me, 2), lax.bitwise_and(me, 3)


def call(kernel, ins, outs, scratch=(), scalars=0, flops=0, limit=8):
    in_specs = [sspec()] * scalars + [vspec()] * (len(ins) - scalars)
    moved = sum(a.size * a.dtype.itemsize for a in list(ins) + list(outs))
    return pl.pallas_call(
        kernel,
        out_shape=tuple(outs),
        in_specs=in_specs,
        out_specs=tuple(vspec() for _ in outs),
        scratch_shapes=list(scratch),
        cost_estimate=pl.CostEstimate(flops=flops, transcendentals=0, bytes_accessed=moved),
        compiler_params=pltpu.CompilerParams(vmem_limit_bytes=limit << 20),
    )(*ins)


def split_kernel(live_ref, q_hbm, k_hbm, v_hbm, *refs, outer, width, groups, copies):
    _, z, r = place()
    q_outs = refs[:INNER]
    kv_outs = refs[INNER:INNER + len(groups)]
    q_ref, k_ref, v_ref, sems = refs[INNER + len(groups):]
    keys = k_ref.shape[0]
    loads = [
        pltpu.make_async_copy(source, target, sems.at[i])
        for i, (source, target) in enumerate(((q_hbm, q_ref), (k_hbm, k_ref), (v_hbm, v_ref)))
    ]
    for load in loads:
        load.start()
    live = jnp.full((8, HEAD_SIZE), live_ref[0], jnp.int32).astype(f32).astype(bf16)
    loads[0].wait()
    for k, out in enumerate(q_outs):
        for zz in range(outer):
            col = pl.multiple_of((zz * INNER + lax.bitwise_xor(r, k)) * width, width)
            out[zz] = q_ref[:, pl.ds(col, width)]
    loads[1].wait()
    loads[2].wait()
    for (k, offsets), out in zip(groups, kv_outs):
        for i, kk in enumerate(offsets):
            head = lax.bitwise_xor(z, kk) * INNER + lax.bitwise_xor(r, k)
            col = pl.multiple_of((head // copies) * HEAD_SIZE, HEAD_SIZE)
            out[i, 0:keys, :] = k_ref[:, pl.ds(col, HEAD_SIZE)]
            out[i, keys:2 * keys, :] = v_ref[:, pl.ds(col, HEAD_SIZE)]
            out[i, 2 * keys:2 * keys + 8, :] = live


def split_weight_kernel(w_ref, out_ref):
    _, _, r = place()
    half = out_ref.shape[1]
    col = pl.multiple_of((1 - lax.bitwise_and(r, 1)) * half, 128)
    out_ref[...] = w_ref[:, pl.ds(col, half)]


def attention_kernel(first_ref, *refs, outer, begin, offsets, rows_all, keys, heads, width):
    ys = refs[:outer]
    kvs = refs[outer:outer + INNER]
    outs = refs[outer + INNER:outer + INNER + len(offsets)]
    bias_ref, q_ref = refs[outer + INNER + len(offsets):]
    _, z, r = place()
    rows = rows_all // (outer * INNER)
    q_pos = first_ref[0] + lax.broadcasted_iota(jnp.int32, (rows_all, keys), 0)
    lane = lax.broadcasted_iota(jnp.int32, (rows_all, keys), 1)
    lane_f = lane.astype(f32)
    for k in range(INNER):
        start = (z * INNER + lax.bitwise_xor(r, k)) * keys
        live = kvs[k][0, 2 * keys:2 * keys + 1, :].astype(f32)
        live = jnp.concatenate([live] * (keys // HEAD_SIZE), axis=1)
        allowed = (lane_f < live) & (start + lane <= q_pos)
        bias_ref[:, k * keys:(k + 1) * keys] = jnp.where(allowed, 0.0, masked_value)
    column = lax.broadcasted_iota(jnp.int32, (rows_all, 128), 1)
    for i, kk in enumerate(offsets):
        zz = lax.bitwise_xor(z, kk)
        for k2 in range(outer):
            for k in range(INNER):
                src = lax.bitwise_xor(z, k2) * INNER + lax.bitwise_xor(r, k)
                at = pl.multiple_of(src * rows, rows)
                q_ref[pl.ds(at, rows), :] = ys[k2][k, zz].astype(f32)
        stats = jnp.zeros((rows_all, 128), f32)
        for h in range(heads):
            cols = slice(h * HEAD_SIZE, (h + 1) * HEAD_SIZE)
            query = q_ref[:, cols].astype(bf16)
            scores = []
            for k in range(INNER):
                part = lax.dot_general(
                    query, kvs[k][begin[k] + i, 0:keys, :], (((1,), (1,)), ((), ())),
                    preferred_element_type=f32,
                )
                scores.append(part * (score_scale * log2e) + bias_ref[:, k * keys:(k + 1) * keys])
            top = functools.reduce(jnp.maximum, scores)
            best = jnp.maximum(jnp.max(top, axis=1, keepdims=True), -1e29)
            acc = jnp.zeros((rows_all, HEAD_SIZE), f32)
            sums = jnp.zeros((rows_all, keys), f32)
            for k in range(INNER):
                weights = jnp.exp2(scores[k] - best)
                sums = sums + weights
                acc = acc + jnp.dot(
                    weights.astype(bf16), kvs[k][begin[k] + i, keys:2 * keys, :], preferred_element_type=f32
                )
            total = jnp.sum(sums, axis=1, keepdims=True)
            safe = jnp.where(total > 0, total, 1.0)
            outs[i][0:rows_all, cols] = (acc / safe).astype(bf16)
            logsum = jnp.where(total > 0, best * ln2 + jnp.log(safe), masked_value)
            high = logsum.astype(bf16).astype(f32)
            rest = logsum - high
            mid = rest.astype(bf16).astype(f32)
            low = rest - mid
            for p, piece in enumerate((high, mid, low)):
                stats = jnp.where(column == p * heads + h, piece, stats)
        turned = stats.T
        pieces = rows_all // width
        per = 8 // pieces
        block = [turned[0:per, j * width:(j + 1) * width] for j in range(pieces)]
        block = block[0] if pieces == 1 else jnp.concatenate(block, axis=0)
        outs[i][rows_all:rows_all + 8, :] = block.astype(bf16)


def merge_kernel(*refs, sources, rows_all, heads, width):
    parts = refs[:sources]
    out, turn_ref = refs[sources:]
    pieces = rows_all // width
    per = 8 // pieces
    logs = []
    for part in parts:
        block = part[rows_all:rows_all + 8, :].astype(f32)
        block = [block[j * per:(j + 1) * per] for j in range(pieces)]
        block = block[0] if pieces == 1 else jnp.concatenate(block, axis=1)
        logs.append(block[0:heads] + (block[heads:2 * heads] + block[2 * heads:3 * heads]))
    top = functools.reduce(jnp.maximum, logs)
    scales = [jnp.exp(l - top) for l in logs]
    total = functools.reduce(jnp.add, scales)
    turn_ref[...] = jnp.zeros_like(turn_ref)
    for i, scale in enumerate(scales):
        turn_ref[i * heads:(i + 1) * heads, :] = scale / total
    turned = turn_ref[...].T
    for h in range(heads):
        cols = slice(h * HEAD_SIZE, (h + 1) * HEAD_SIZE)
        acc = jnp.zeros((rows_all, HEAD_SIZE), f32)
        for i, part in enumerate(parts):
            at = i * heads + h
            acc = acc + turned[:, at:at + 1] * part[0:rows_all, cols].astype(f32)
        out[:, cols] = acc.astype(bf16)


def project_kernel(
    mine_ref, other_ref, w_mine_ref, w_other_ref, *out_refs, order, outer, rows, early, blocks
):
    _, z, r = place()
    y = lax.shift_right_logical(r, 1)
    half = w_other_ref.shape[1]
    sends, keeps, earlies = out_refs[:outer], out_refs[outer:2 * outer], out_refs[2 * outer:]
    span = 2 * rows
    far = [kk for kk in order if kk >= outer // 2]

    def gather(picks):
        found = []
        for ref in (mine_ref, other_ref):
            lines = []
            for kk, first, size in picks:
                at = (lax.bitwise_xor(z, kk) * INNER + first) * rows
                lines.append(ref[pl.ds(pl.multiple_of(at, size), size), :])
            found.append(jnp.concatenate(lines, axis=0))
        return found

    def terms(lines, begin, cols):
        col = pl.multiple_of(lax.bitwise_and(r, 1) * half + begin, 128)
        term = jnp.dot(lines[0], w_mine_ref[:, pl.ds(col, cols)], preferred_element_type=f32)
        return term + jnp.dot(
            lines[1], w_other_ref[:, begin:begin + cols], preferred_element_type=f32
        )

    sides = [(2 * (1 - y), sends), (2 * y, keeps)]
    lines = gather([(kk, first, span) for first, outs in sides for kk in order])
    cols = (half - early) // blocks
    for j in range(blocks):
        term = terms(lines, early + j * cols, cols)
        for i, out in enumerate(sends + keeps):
            at = j * cols + out.shape[1] - (half - early)
            out[:, at:at + cols] = term[i * span:(i + 1) * span].astype(out.dtype)
    near = [(kk, first, outs[i]) for first, outs in sides for i, kk in enumerate(order)
            if kk not in far]
    picks = [(kk, 0, 2 * span) for kk in far] + [(kk, first, span) for kk, first, out in near]
    term = terms(gather(picks), 0, early)
    at = 0
    for out in list(earlies) + [out for kk, first, out in near]:
        out[:, 0:early] = term[at:at + out.shape[0]].astype(out.dtype)
        at += out.shape[0]


def first_sum_kernel(keep_ref, got_ref, out_ref):
    out_ref[...] = (keep_ref[...] + got_ref[...].astype(f32)).astype(out_ref.dtype)


def early_sum_kernel(*refs, span):
    *parts, send_ref, keep_ref, total_ref = refs
    _, _, r = place()
    y = lax.shift_right_logical(r, 1)
    total_ref[...] = functools.reduce(jnp.add, [part[...].astype(f32) for part in parts])
    send_ref[...] = total_ref[pl.ds(pl.multiple_of((1 - y) * span, span), span), :].astype(bf16)
    keep_ref[...] = total_ref[pl.ds(pl.multiple_of(y * span, span), span), :]


def last_sum_kernel(early_keep_ref, early_got_ref, keep_ref, got_ref, *refs, rows):
    *parts, mine_ref, other_ref, total_ref = refs
    _, _, r = place()
    c = lax.bitwise_and(r, 1)
    early = early_keep_ref.shape[1]
    half = keep_ref.shape[1]
    total = keep_ref[...] + got_ref[...].astype(f32)
    for part in parts:
        if part.shape[1] == half:
            total = total + part[...].astype(f32)
    total_ref[:, :early] = total[:, :early] + early_keep_ref[...] + early_got_ref[...].astype(f32)
    total = total[:, early:]
    for part in parts:
        if part.shape[1] != half:
            total = total + part[...].astype(f32)
    total_ref[:, early:] = total
    mine_ref[...] = total_ref[pl.ds(pl.multiple_of(c * rows, rows), rows), :].astype(bf16)
    other_ref[...] = total_ref[pl.ds(pl.multiple_of((1 - c) * rows, rows), rows), :].astype(bf16)


def join_kernel(mine_ref, other_ref, out_ref):
    _, _, r = place()
    c = lax.bitwise_and(r, 1)
    half = mine_ref.shape[1]
    out_ref[:, pl.ds(pl.multiple_of(c * half, 128), half)] = mine_ref[...]
    out_ref[:, pl.ds(pl.multiple_of((1 - c) * half, 128), half)] = other_ref[...]


def layer(query_block, cache_keys, stored_values, live_counts, first_position, out_weight):
    devices = lax.axis_size("seq")
    outer = devices // INNER
    rows = query_block.shape[0]
    rows_all = rows * devices
    keys = cache_keys.shape[0]
    heads = QUERY_HEADS // devices
    width = heads * HEAD_SIZE
    copies = devices // KEY_VALUE_HEADS
    model = out_weight.shape[1]
    half = model // 2
    assert heads * copies == QUERY_HEADS // KEY_VALUE_HEADS and keys <= 256
    tiles = half // 128
    early = 128 * (tiles * EARLY_PART // 100)
    blocks = next(b for b in (2, 3, 1) if (half - early) % (128 * b) == 0)
    shape = jax.ShapeDtypeStruct

    def swap(x, k):
        return lax.ppermute(x, "seq", [(i, i ^ k) for i in range(devices)])

    order = [outer - 1, 1] + list(range(outer - 2, 1, -1)) + [0]
    phases = [order[:outer // 2], order[outer // 2:3 * outer // 4], order[3 * outer // 4:]]
    groups = [(0, order), (1, order)] + [(k, p) for p in phases for k in range(2, INNER)]
    inputs = [
        pltpu.with_memory_space_constraint(x, pltpu.MemorySpace.HBM)
        for x in (query_block, cache_keys, stored_values)
    ]
    outs = [shape((outer, rows, width), bf16)] * INNER
    outs += [shape((len(p), 2 * keys + 8, HEAD_SIZE), bf16) for k, p in groups]
    split = pl.pallas_call(
        functools.partial(split_kernel, outer=outer, width=width, groups=groups, copies=copies),
        out_shape=tuple(outs),
        in_specs=[sspec()] + [pl.BlockSpec(memory_space=pltpu.MemorySpace.HBM)] * 3,
        out_specs=tuple(vspec() for _ in outs),
        scratch_shapes=[pltpu.VMEM(x.shape, x.dtype) for x in inputs]
        + [pltpu.SemaphoreType.DMA((3,))],
        name="split",
        compiler_params=pltpu.CompilerParams(vmem_limit_bytes=8 << 20),
    )(live_counts, *inputs)
    q_out, kv_out = split[:INNER], split[INNER:]
    q_got = {k: swap(q_out[k], k) for k in (2, 3, 1)}
    kv_pair = swap(kv_out[1], 1)
    kv_far = [
        {k: swap(kv_out[2 + 2 * i + k - 2], k) for k in range(2, INNER)}
        for i in range(len(phases))
    ]
    inner_q = jnp.stack([q_out[0], q_got[1], q_got[2], q_got[3]])
    ys = [inner_q] + [swap(inner_q, k * INNER) for k in range(1, outer)]

    (w_send,) = call(
        split_weight_kernel, [out_weight],
        [shape((out_weight.shape[0], half), bf16)],
    )
    w_other = swap(w_send, 1)

    partial_of = {}
    for near, kk in enumerate(order):
        i = [kk in p for p in phases].index(True)
        far = phases[i].index(kk)
        (out,) = call(
            functools.partial(
                attention_kernel, outer=outer, begin=(near, near) + (far,) * (INNER - 2),
                offsets=[kk], rows_all=rows_all, keys=keys, heads=heads, width=width,
            ),
            [first_position, *ys, kv_out[0], kv_pair, kv_far[i][2], kv_far[i][3]],
            [shape((rows_all + 8, width), bf16)],
            scratch=[pltpu.VMEM((rows_all, INNER * keys), f32), pltpu.VMEM((rows_all, width), f32)],
            scalars=1, flops=4 * rows_all * INNER * keys * width, limit=16,
        )
        partial_of[kk] = swap(out, kk * INNER) if kk else out

    (merged,) = call(
        functools.partial(merge_kernel, sources=outer, rows_all=rows_all, heads=heads, width=width),
        [partial_of[k] for k in range(outer)], [shape((rows_all, width), bf16)],
        scratch=[pltpu.VMEM((128, rows_all), f32)],
    )
    other = swap(merged, 1)

    span = 2 * rows
    far = [kk for kk in order if kk >= outer // 2]
    widths = [half - early if kk in far else half for kk in order]
    terms = call(
        functools.partial(
            project_kernel, order=order, outer=outer, rows=rows, early=early, blocks=blocks
        ),
        [merged, other, out_weight, w_other],
        [shape((span, w), bf16) for w in widths] + [shape((span, w), f32) for w in widths]
        + [shape((2 * span, early), bf16)] * len(far),
        flops=4 * rows_all * width * half, limit=20,
    )
    sends, keeps, earlies = terms[:outer], terms[outer:2 * outer], terms[2 * outer:]
    gots = [swap(x, 2) for x in sends]
    early_gots = [swap(x, kk * INNER) for kk, x in zip(far, earlies)]
    parts = []
    for i, kk in enumerate(order[:-1]):
        (part,) = call(
            first_sum_kernel, [keeps[i], gots[i]],
            [shape((span, widths[i]), bf16)],
        )
        parts.append(swap(part, kk * INNER))
    early_send, early_keep = call(
        functools.partial(early_sum_kernel, span=span),
        early_gots, [shape((span, early), bf16), shape((span, early), f32)],
        scratch=[pltpu.VMEM((2 * span, early), f32)],
    )
    mine, theirs = call(
        functools.partial(last_sum_kernel, rows=rows),
        [early_keep, swap(early_send, 2), keeps[-1], gots[-1]] + parts,
        [shape((rows, half), bf16)] * 2, scratch=[pltpu.VMEM((span, half), f32)],
    )
    (joined,) = call(join_kernel, [mine, swap(theirs, 1)], [shape((rows, model), bf16)])
    return joined


def solution(mesh):
    in_specs = (
        P(("groups", "seq"), None),
        P(("groups", "seq"), None),
        P(("groups", "seq"), None),
        P(("groups", "seq")),
        P("groups"),
        P("seq", None),
    )
    out_specs = P(("groups", "seq"), None)
    return jax.shard_map(layer, mesh=mesh, in_specs=in_specs, out_specs=out_specs, check_vma=False)
```
